256 devices in a mesh: row: 16 (over x, y), col: 16 (over z, core).
Axes of the slice: x: 4, y: 4, z: 8, core: 2. Of those that a mesh axis runs over, the one named last changes fastest.
Arguments:
- inv_hessian: float32 [12288, 12288], P('row', 'col'), as said below
- weights: bfloat16 [24576, 12288], P('row', 'col'), may hold values from -6 to 6
- calib: bfloat16 [128, 12288], replicated, may hold values from -6 to 6
- block: int32 [1], replicated, may hold values from 0 to 47
Outputs:
- updated: float32 [12288, 12288], P('row', 'col')
- pruned: bfloat16 [24576, 12288], P('row', 'col')
The draws below stay inside these ranges and needn't reach their ends.
Inputs may be any that keep to these rules, and one draw needn't show every extreme that they name: `inv_hessian`: symmetric and positive definite.
All inputs are finite; a program needn't handle non-finite values.
Results may differ from the reference program's by a relative error of at most 0.002.
Values may be sent and summed in bfloat16 or wider, within the bound.
No kernel may reach another device: no remote copies, remote signals or barrier semaphores. Data moves between devices by JAX's collectives and lax.ppermute only.
A program may use at most 128 MiB of HBM per device.

```python
import math
import jax
import jax.numpy as jnp
from jax import lax

D = 12288
FF = 24576
B = 256
CAL = 128


def draw_inv_hessian(key, part):
    base = jax.random.fold_in(key, 17)
    first, second, third, fourth = jax.random.split(base, 4)
    noise = jax.random.normal(first, (D, D), jnp.float32) * (0.35 / math.sqrt(D))
    spread = (noise + noise.T) * 0.7071067811865476
    factor_count = 2 * (D // B)
    owner = jnp.arange(D) // B
    group = jnp.arange(factor_count) // 2
    inside = owner[:, None] == group[None, :]
    local = jnp.where(inside, jax.random.normal(third, (D, factor_count), jnp.float32), 0.0)
    tails = jax.random.normal(fourth, (D, factor_count), jnp.float32) * 0.2
    factors = local + tails
    correlated = 0.15 * jnp.dot(factors, factors.T, precision=lax.Precision.HIGHEST)
    correlated = 0.5 * (correlated + correlated.T)
    diagonal = jnp.exp(jax.random.uniform(second, (D,), jnp.float32, 0.0, math.log(2.5)))
    return spread + correlated + jnp.diag(diagonal)


def level_of(key, dims, shards, least, high):
    loudness, own = 1.0, jax.random.fold_in(key, 6)
    for position, blocks in shards:
        draws = jnp.exp(jax.random.uniform(jax.random.fold_in(own, position), (blocks,), jnp.float32, least / len(shards), high / len(shards)))
        loudness = loudness * jnp.repeat(draws, dims[position] // blocks).reshape([-1 if axis == position else 1 for axis in range(len(dims))])
    return loudness


def normal_values(key, extent, deviation, limit, shards=(), kind=jnp.bfloat16):
    loudness = level_of(key, extent, shards, -0.22, 0.18) if shards else 1.0
    entries = jax.random.normal(key, extent, jnp.float32) * deviation * loudness
    return jnp.minimum(jnp.maximum(entries, -limit), limit).astype(kind)


def setup_inputs(seed: int = 0) -> dict:
    splits = jax.random.split(jax.random.key(seed), 5)
    inv_hessian = draw_inv_hessian(jax.random.fold_in(splits[4], 71), 0)
    weights = normal_values(splits[1], (FF, D), 1.0, 6.0, ((0, 16), (1, 16)))
    calib = normal_values(splits[2], (CAL, D), 1.0, 6.0)
    block = jax.random.randint(splits[3], (1,), 0, D // B).astype(jnp.int32)
    return dict(inv_hessian=inv_hessian, weights=weights, calib=calib, block=block)


def reference(inv_hessian, weights, calib, block):
    highest = lax.Precision.HIGHEST
    calib_f = calib.astype(jnp.float32)
    left = jnp.dot(calib_f, inv_hessian, precision=highest)
    right = jnp.dot(inv_hessian, calib_f.T, precision=highest)
    inner = jnp.eye(CAL, dtype=jnp.float32) + jnp.dot(left, calib_f.T, precision=highest)
    inner = 0.5 * (inner + inner.T)
    factor = jnp.linalg.cholesky(inner)
    solved = jax.scipy.linalg.cho_solve((factor, True), left)
    updated = inv_hessian - jnp.dot(right, solved, precision=highest)
    start = (block[0] * B).astype(jnp.int32)
    strip = lax.dynamic_slice_in_dim(updated, start, B, 0)
    square = lax.dynamic_slice_in_dim(strip, start, B, 1)
    square = 0.5 * (square + square.T)
    square_factor = jnp.linalg.cholesky(square)
    comp = jax.scipy.linalg.cho_solve((square_factor, True), strip).astype(jnp.bfloat16)
    window = lax.dynamic_slice_in_dim(weights, start, B, 1)
    product = jnp.dot(window.astype(jnp.float32), comp.astype(jnp.float32), preferred_element_type=jnp.float32)
    pruned = (weights.astype(jnp.float32) - product).astype(jnp.bfloat16)
    return (updated, pruned)
```

```python
import jax
import jax.numpy as jnp
from jax import lax
from jax.sharding import Mesh
from jax.sharding import PartitionSpec as P

B = 256
COL = ("z", "core")
HIGHEST = lax.Precision.HIGHEST


def exchanged(parts, axis):
    return lax.all_to_all(parts, axis, split_axis=0, concat_axis=0, tiled=True)


def from_everyone(x, axis):
    return exchanged(jnp.broadcast_to(x, (lax.axis_size(axis), *x.shape)), axis)


def picked(parts, root):
    return lax.dynamic_index_in_dim(parts, root, 0, keepdims=False)


def from_all_columns(x):
    return from_everyone(from_everyone(x, "z"), "core")


def per_device(inv_hessian, weights, calib, block):
    tile_rows, tile = inv_hessian.shape
    peers = lax.axis_size("row")
    row = lax.axis_index("row")
    col = lax.axis_index(COL)
    start = block[0] * B
    owner = start // tile
    sub = (start - owner * tile) // B
    offset = sub * B
    groups = tile // B
    wide = tile // 128

    window = lax.dynamic_slice_in_dim(weights, offset, B, 1)
    lines = window.shape[0] // peers
    scattered = exchanged(window.reshape(2, -1, B), "core")
    scattered = picked(scattered.reshape(2, -1, B), owner % 2)
    scattered = exchanged(scattered.reshape(8, lines, B), "z")
    window_piece = picked(scattered, owner // 2)

    calib_rows = lax.dynamic_slice_in_dim(calib, row * tile_rows, tile_rows, 1).astype(jnp.float32)
    calib_cols = lax.dynamic_slice_in_dim(calib, col * tile, tile, 1).astype(jnp.float32)
    left_part = jnp.dot(calib_rows, inv_hessian, precision=HIGHEST)
    inner_part = jnp.dot(left_part, calib_cols.T, precision=HIGHEST)
    part = left_part.T
    strip = lax.dynamic_slice_in_dim(inv_hessian, offset, B, 0)
    thin = B // peers
    sent = jnp.concatenate(
        [
            part.reshape(groups, peers, thin, 128).swapaxes(0, 1).reshape(peers, -1, 128),
            inner_part.reshape(peers, -1, 128),
            strip.reshape(peers, thin, wide, 128).swapaxes(1, 2).reshape(peers, -1, 128),
        ],
        axis=1,
    )
    arrived = exchanged(sent, "row")
    piece_rows = groups * thin
    inner_rows = 128 // peers
    summed = arrived[:, : piece_rows + inner_rows].sum(axis=0)
    piece = summed[:piece_rows]
    strip_piece = picked(arrived, owner)[piece_rows + inner_rows :]

    n = peers
    turn = [(i * n + j, j * n + i) for i in range(n) for j in range(n)]
    turned = lax.ppermute(piece, ("row", *COL), turn)
    mine = picked(piece.reshape(groups, thin, 128), sub)
    mine_square = lax.dynamic_slice_in_dim(strip_piece.reshape(wide, thin, 128), 2 * sub, 2, 0)
    small = jnp.concatenate([summed[piece_rows:], mine, mine_square.reshape(-1, 128)], axis=0)
    small = lax.all_gather(small, COL)
    small = jnp.concatenate(
        [small[:, :inner_rows].sum(axis=0), picked(small, owner)[inner_rows:]], axis=0
    )
    large = from_everyone(jnp.concatenate([piece, strip_piece], axis=0), "row")
    small = from_everyone(small, "row")
    inner = small[:, :inner_rows].reshape(128, 128)
    block_right = small[:, inner_rows : inner_rows + thin].reshape(B, 128)
    square = small[:, inner_rows + thin :].reshape(peers, 2, thin, 128)
    square = square.swapaxes(1, 2).reshape(B, B)
    right_cols = large[:, :piece_rows].reshape(peers, groups, thin, 128)
    right_cols = right_cols.swapaxes(0, 1).reshape(tile, 128)
    strip = large[:, piece_rows:].reshape(peers, wide, thin, 128).swapaxes(1, 2).reshape(B, tile)

    right_rows = from_all_columns(turned).swapaxes(0, 1).reshape(peers, groups, thin, 128)
    right_rows = right_rows.swapaxes(0, 1).reshape(tile_rows, 128)
    window = from_all_columns(window_piece).reshape(window.shape)

    inner = jnp.eye(128, dtype=jnp.float32) + 0.5 * (inner + inner.T)
    factor = jnp.linalg.cholesky(inner)
    both = jnp.concatenate([block_right, right_cols], axis=0).T
    solved = jax.scipy.linalg.cho_solve((factor, True), both)
    changed = jnp.dot(block_right, solved, precision=HIGHEST)
    square = square - changed[:, :B]
    strip = strip - changed[:, B:]
    updated = inv_hessian - jnp.dot(right_rows, solved[:, B:], precision=HIGHEST)
    square = 0.5 * (square + square.T)
    square_factor = jnp.linalg.cholesky(square)
    comp = jax.scipy.linalg.cho_solve((square_factor, True), strip).astype(jnp.bfloat16)
    product = jnp.dot(window, comp, preferred_element_type=jnp.float32)
    pruned = (weights.astype(jnp.float32) - product).astype(jnp.bfloat16)
    return (updated, pruned)


def solution(mesh):
    finer = Mesh(mesh.devices.reshape(mesh.shape["row"], 8, 2), ("row", "z", "core"))
    specs = (P("row", COL), P("row", COL), P(), P())
    return jax.shard_map(
        per_device, mesh=finer, in_specs=specs, out_specs=specs[:2], check_vma=False
    )
```

```python
import jax
import jax.numpy as jnp
from jax import lax
from jax.experimental import pallas as pl
from jax.experimental.pallas import tpu as pltpu
from jax.sharding import Mesh
from jax.sharding import PartitionSpec as P

B = 256
L = 128
COL = ("z", "core")
F32 = jnp.float32
BF16 = jnp.bfloat16
HIGHEST = lax.Precision.HIGHEST


def exchanged(parts, axis):
    return lax.all_to_all(parts, axis, split_axis=0, concat_axis=0, tiled=True)


def dot(a, b, dims=((1,), (0,))):
    return lax.dot_general(a, b, (dims, ((), ())), precision=HIGHEST, preferred_element_type=F32)


def dot_nt(a, b):
    return dot(a, b, ((1,), (1,)))


def in_three(x):
    first = x.astype(BF16)
    rest = x - first.astype(F32)
    second = rest.astype(BF16)
    third = (rest - second.astype(F32)).astype(BF16)
    return first, second, third


def place_of(block_ref, groups):
    owner = block_ref[0] // groups
    return owner, block_ref[0] - owner * groups


def first_kernel(block_ref, h_ref, calib_ref, w_ref, sent_ref, window_ref, rows_ref, cols_ref, sems):
    n, lines, _ = window_ref.shape
    tile = h_ref.shape[1]
    groups, wide, thin = tile // B, tile // L, B // n
    _, sub = place_of(block_ref, groups)
    row = lax.axis_index("row")
    col = lax.axis_index("z") * lax.axis_size("core") + lax.axis_index("core")
    offset = pl.multiple_of(sub * B, B)
    copies = [
        pltpu.make_async_copy(
            calib_ref.at[:, pl.ds(pl.multiple_of(row * tile, L), tile)], rows_ref, sems.at[0]
        ),
        pltpu.make_async_copy(
            calib_ref.at[:, pl.ds(pl.multiple_of(col * tile, L), tile)], cols_ref, sems.at[1]
        ),
        pltpu.make_async_copy(w_ref.at[:, :, pl.ds(offset, B)], window_ref, sems.at[2]),
    ]
    for copy in copies:
        copy.start()
    copies[0].wait()
    copies[1].wait()
    first, second, third = in_three(h_ref[...])
    rows = rows_ref[...]
    left = jnp.dot(rows, first, preferred_element_type=F32)
    left += jnp.dot(rows, second, preferred_element_type=F32)
    left += jnp.dot(rows, third, preferred_element_type=F32)
    right = left.T
    cols = cols_ref[...]
    dims = (((1,), (1,)), ((), ()))
    first, second, third = in_three(left)
    inner = lax.dot_general(first, cols, dims, preferred_element_type=F32)
    inner += lax.dot_general(second, cols, dims, preferred_element_type=F32)
    inner += lax.dot_general(third, cols, dims, preferred_element_type=F32)
    cut = L // n
    for p in range(n):
        for s in range(groups):
            at = s * B + p * thin
            sent_ref[p, s * thin : (s + 1) * thin, :] = right[at : at + thin]
        at = groups * thin
        sent_ref[p, at : at + cut, :] = inner[p * cut : (p + 1) * cut]
        at += cut
        for w in range(wide):
            sent_ref[p, at + w * thin : at + (w + 1) * thin, :] = h_ref[
                pl.ds(pl.multiple_of(offset + p * thin, thin), thin), w * L : (w + 1) * L
            ]
    copies[2].wait()


def second_kernel(block_ref, arrived_ref, small_ref, piece_ref, strip_ref):
    n = arrived_ref.shape[0]
    rows = piece_ref.shape[0]
    thin, cut = B // n, L // n
    owner, sub = place_of(block_ref, rows // thin)
    total = arrived_ref[0, 0 : rows + cut, :]
    for p in range(1, n):
        total = total + arrived_ref[p, 0 : rows + cut, :]
    piece_ref[...] = total[:rows]
    strip_ref[...] = arrived_ref[owner, rows + cut :, :]
    small_ref[0:cut] = total[rows:]
    small_ref[cut : cut + thin] = piece_ref[pl.ds(pl.multiple_of(sub * thin, thin), thin), :]
    small_ref[cut + thin :] = strip_ref[
        pl.ds(pl.multiple_of(2 * sub * thin, 2 * thin), 2 * thin), :
    ]


def third_kernel(block_ref, gathered_ref, piece_ref, strip_ref, sent_ref, right_ref):
    n = gathered_ref.shape[0]
    rows = piece_ref.shape[0]
    thin, cut = B // n, L // n
    groups = rows // thin
    owner, _ = place_of(block_ref, groups)
    small = gathered_ref.shape[1] - rows
    total = gathered_ref[0, 0:cut, :]
    for p in range(1, n):
        total = total + gathered_ref[p, 0:cut, :]
    chosen = gathered_ref[owner, cut:small, :]
    piece, strip = piece_ref[...], strip_ref[...]
    for p in range(n):
        sent_ref[p, 0:cut, :] = total
        sent_ref[p, cut:small, :] = chosen
        sent_ref[p, small : small + rows, :] = piece
        sent_ref[p, small + rows :, :] = strip
        for s in range(groups):
            at = s * B + p * thin
            right_ref[at : at + thin, :] = gathered_ref[
                p, small + s * thin : small + (s + 1) * thin, :
            ]


def invert(a_ref):
    lane = lax.broadcasted_iota(jnp.int32, (8, L), 1)
    sub = lax.broadcasted_iota(jnp.int32, (8, L), 0)
    wide_lane = lax.broadcasted_iota(jnp.int32, (L, L), 1)

    def step(k, carry):
        base = pl.multiple_of(8 * k, 8)
        panel = a_ref[pl.ds(base, 8), :]
        columns = [
            jnp.broadcast_to(
                jnp.sum(jnp.where(lane == base + j, panel, 0.0), axis=1, keepdims=True), (8, L)
            )
            for j in range(8)
        ]
        whole = a_ref[...]
        factors = [
            jnp.sum(jnp.where(wide_lane == base + j, whole, 0.0), axis=1, keepdims=True)
            for j in range(8)
        ]
        for j in range(8):
            own = columns[j]
            inverse = 1.0 / own[j : j + 1, :]
            here = sub == j
            panel = jnp.where(lane == base + j, jnp.where(here, 1.0, 0.0), panel)
            scaled = panel[j : j + 1, :] * inverse
            panel = jnp.where(here, scaled, panel - own * scaled)
            for m in range(j + 1, 8):
                scaled = columns[m][j : j + 1, :] * inverse
                columns[m] = jnp.where(here, scaled, columns[m] - own * scaled)
        inside = (wide_lane >= base) & (wide_lane < base + 8)
        rest = jnp.where(inside, 0.0, whole)
        for j in range(8):
            rest = rest - factors[j] * panel[j : j + 1, :]
        a_ref[...] = rest
        a_ref[pl.ds(base, 8), :] = panel
        return carry

    lax.fori_loop(0, L // 8, step, 0)


def fourth_kernel(c_ref, solved_ref, comp_ref, a_ref, gm_ref, gc_ref, q_ref, st_ref):
    n = c_ref.shape[0]
    tile = gc_ref.shape[0]
    thin, cut, groups, wide = B // n, L // n, tile // B, tile // L
    for p in range(n):
        a_ref[p * cut : (p + 1) * cut, :] = c_ref[p, 0:cut, :]
        at = cut
        gm_ref[p * thin : (p + 1) * thin, :] = c_ref[p, at : at + thin, :]
        at += thin
        for w in range(2):
            q_ref[p * thin : (p + 1) * thin, w * L : (w + 1) * L] = c_ref[p, at : at + thin, :]
            at += thin
        for s in range(groups):
            gc_ref[s * B + p * thin : s * B + (p + 1) * thin, :] = c_ref[p, at : at + thin, :]
            at += thin
        for w in range(wide):
            st_ref[p * thin : (p + 1) * thin, w * L : (w + 1) * L] = c_ref[p, at : at + thin, :]
            at += thin
    inner = a_ref[...]
    same = lax.broadcasted_iota(jnp.int32, (L, L), 0) == lax.broadcasted_iota(
        jnp.int32, (L, L), 1
    )
    a_ref[...] = jnp.where(same, 1.0, 0.0) + 0.5 * (inner + inner.T)
    invert(a_ref)
    x = a_ref[...]
    block_right = gm_ref[...]
    right = gc_ref[...]
    half = dot(block_right, x)
    solved_ref[...] = dot(right, x)
    square = q_ref[...] - dot_nt(half, block_right)
    square = 0.5 * (square + square.T)
    a_ref[...] = square[:L, :L]
    st_ref[...] = st_ref[...] - dot_nt(half, right)
    invert(a_ref)
    u = a_ref[...]
    v = dot(square[L:, :L], u)
    a_ref[...] = square[L:, L:] - dot(v, square[:L, L:])
    top = st_ref[0:L, :]
    first = dot(u, top)
    second = st_ref[L:, :] - dot(v, top)
    invert(a_ref)
    second = dot(a_ref[...], second)
    comp_ref[0:L, :] = (first - dot(v.T, second)).astype(BF16)
    comp_ref[L:, :] = second.astype(BF16)


VMEM = pl.BlockSpec(memory_space=pltpu.VMEM)
PARAMS = pltpu.CompilerParams(vmem_limit_bytes=20 * 2**20)
SMEM = pl.BlockSpec(memory_space=pltpu.SMEM)
HBM = pl.BlockSpec(memory_space=pltpu.HBM)


def of(shape, dtype=F32):
    return jax.ShapeDtypeStruct(shape, dtype)


def per_device(inv_hessian, weights, calib, block):
    tile = inv_hessian.shape[0]
    n = lax.axis_size("row")
    lines = weights.shape[0] // n
    thin, cut, groups, wide = B // n, L // n, tile // B, tile // L
    rows = groups * thin
    strip_rows = wide * thin
    small_rows = cut + 3 * thin
    sent, window = pl.pallas_call(
        first_kernel,
        out_shape=(of((n, rows + cut + strip_rows, L)), of((n, lines, B), BF16)),
        in_specs=[SMEM, VMEM, HBM, HBM],
        out_specs=(VMEM, HBM),
        scratch_shapes=[
            pltpu.VMEM((L, tile), BF16),
            pltpu.VMEM((L, tile), BF16),
            pltpu.SemaphoreType.DMA((3,)),
        ],
        compiler_params=PARAMS,
        name="first",
    )(block, inv_hessian, calib, weights.reshape(n, lines, tile))
    arrived = exchanged(sent, "row")
    scattered = exchanged(window, COL)
    small, piece, strip = pl.pallas_call(
        second_kernel,
        out_shape=(of((small_rows, L)), of((rows, L)), of((strip_rows, L))),
        in_specs=[SMEM, VMEM],
        out_specs=(VMEM, VMEM, VMEM),
        compiler_params=PARAMS,
        name="second",
    )(block, arrived)
    turn = [(i * n + j, j * n + i) for i in range(n) for j in range(n)]
    turned = lax.ppermute(piece, ("row", *COL), turn)
    gathered = lax.all_gather(jnp.concatenate([small, turned], axis=0), COL)
    sent, right_rows = pl.pallas_call(
        third_kernel,
        out_shape=(of((n, small_rows + rows + strip_rows, L)), of((tile, L))),
        in_specs=[SMEM, VMEM, VMEM, VMEM],
        out_specs=(VMEM, VMEM),
        compiler_params=PARAMS,
        name="third",
    )(block, gathered, piece, strip)
    arrived = exchanged(sent, "row")
    owner = block[0] // groups
    window = lax.dynamic_index_in_dim(scattered, owner, 0, keepdims=False)
    window = exchanged(jnp.broadcast_to(window, (n, lines, B)), COL).reshape(n * lines, B)
    solved, comp = pl.pallas_call(
        fourth_kernel,
        out_shape=(of((tile, L)), of((B, tile), BF16)),
        in_specs=[VMEM],
        out_specs=(VMEM, VMEM),
        scratch_shapes=[
            pltpu.VMEM((L, L), F32),
            pltpu.VMEM((B, L), F32),
            pltpu.VMEM((tile, L), F32),
            pltpu.VMEM((B, B), F32),
            pltpu.VMEM((B, tile), F32),
        ],
        cost_estimate=pl.CostEstimate(
            flops=20_000_000_000, bytes_accessed=4_000_000, transcendentals=0
        ),
        compiler_params=PARAMS,
        name="fourth",
    )(arrived)
    updated = inv_hessian - dot_nt(right_rows, solved)
    product = jnp.dot(window, comp, preferred_element_type=F32)
    pruned = (weights.astype(F32) - product).astype(BF16)
    return (updated, pruned)


def solution(mesh):
    finer = Mesh(mesh.devices.reshape(mesh.shape["row"], 8, 2), ("row", "z", "core"))
    specs = (P("row", COL), P("row", COL), P(), P())
    return jax.shard_map(
        per_device, mesh=finer, in_specs=specs, out_specs=specs[:2], check_vma=False
    )
```

```python
from functools import partial

import jax
import jax.numpy as jnp
from jax import lax
from jax.experimental import pallas as pl
from jax.experimental.pallas import tpu as pltpu
from jax.sharding import Mesh
from jax.sharding import PartitionSpec as P

B = 256
L = 128
ROW = ("x", "y")
COL = ("z", "core")
F32 = jnp.float32
BF16 = jnp.bfloat16
HIGHEST = lax.Precision.HIGHEST


def exchanged(parts, axis):
    return lax.all_to_all(parts, axis, split_axis=0, concat_axis=0, tiled=True)


def dot(a, b, dims=((1,), (0,))):
    return lax.dot_general(a, b, (dims, ((), ())), precision=HIGHEST, preferred_element_type=F32)


def dot_nt(a, b):
    return dot(a, b, ((1,), (1,)))


def in_three(x):
    first = x.astype(BF16)
    rest = x - first.astype(F32)
    second = rest.astype(BF16)
    third = (rest - second.astype(F32)).astype(BF16)
    return first, second, third


def place_of(block_ref, groups):
    owner = block_ref[0] // groups
    return owner, block_ref[0] - owner * groups


def first_kernel(
    block_ref, h_ref, calib_ref, w_ref, sent_ref, keep_ref, give_ref, rows_ref, cols_ref, sems
):
    n = sent_ref.shape[0]
    half = keep_ref.shape[0]
    tile = h_ref.shape[1]
    groups, wide, thin = tile // B, tile // L, B // n
    _, sub = place_of(block_ref, groups)
    row = lax.axis_index("x") * lax.axis_size("y") + lax.axis_index("y")
    core = lax.axis_index("core")
    col = lax.axis_index("z") * lax.axis_size("core") + core
    offset = pl.multiple_of(sub * B, B)

    def window_of(which):
        return w_ref.at[pl.ds(which * half, half), :, pl.ds(offset, B)]

    copies = [
        pltpu.make_async_copy(
            calib_ref.at[:, pl.ds(pl.multiple_of(row * tile, L), tile)], rows_ref, sems.at[0]
        ),
        pltpu.make_async_copy(
            calib_ref.at[:, pl.ds(pl.multiple_of(col * tile, L), tile)], cols_ref, sems.at[1]
        ),
        pltpu.make_async_copy(window_of(core), keep_ref, sems.at[2]),
        pltpu.make_async_copy(window_of(1 - core), give_ref, sems.at[3]),
    ]
    for copy in copies:
        copy.start()
    copies[0].wait()
    copies[1].wait()
    first, second, third = in_three(h_ref[...])
    rows = rows_ref[...]
    left = jnp.dot(rows, first, preferred_element_type=F32)
    left += jnp.dot(rows, second, preferred_element_type=F32)
    left += jnp.dot(rows, third, preferred_element_type=F32)
    right = left.T
    cols = cols_ref[...]
    dims = (((1,), (1,)), ((), ()))
    first, second, third = in_three(left)
    inner = lax.dot_general(first, cols, dims, preferred_element_type=F32)
    inner += lax.dot_general(second, cols, dims, preferred_element_type=F32)
    inner += lax.dot_general(third, cols, dims, preferred_element_type=F32)
    cut = L // n
    for p in range(n):
        for s in range(groups):
            at = s * B + p * thin
            sent_ref[p, s * thin : (s + 1) * thin, :] = right[at : at + thin]
        at = groups * thin
        sent_ref[p, at : at + cut, :] = inner[p * cut : (p + 1) * cut]
        at += cut
        for w in range(wide):
            sent_ref[p, at + w * thin : at + (w + 1) * thin, :] = h_ref[
                pl.ds(pl.multiple_of(offset + p * thin, thin), thin), w * L : (w + 1) * L
            ]
    copies[2].wait()
    copies[3].wait()


def choose_kernel(block_ref, keep_ref, got_ref, *turned_refs, groups):
    count = len(turned_refs)
    owner, _ = place_of(block_ref, groups)
    z = lax.axis_index("z")
    own = owner % 2 == lax.axis_index("core")
    for k in range(count):
        at = (z + k) % count
        turned_refs[k][...] = jnp.where(own, keep_ref[at], got_ref[at])


def second_kernel(block_ref, arrived_ref, *refs):
    *shifted, small_ref, piece_ref, sent_ref, window_ref = refs
    n = arrived_ref.shape[0]
    rows = piece_ref.shape[0]
    thin, cut = B // n, L // n
    owner, sub = place_of(block_ref, rows // thin)
    z = lax.axis_index("z")
    for k, ref in enumerate(shifted):

        @pl.when((z + len(shifted) - owner // 2) % len(shifted) == k)
        def _(ref=ref):
            window_ref[...] = ref[...]

    total = arrived_ref[0, 0 : rows + cut, :]
    for p in range(1, n):
        total = total + arrived_ref[p, 0 : rows + cut, :]
    piece = total[:rows]
    strip = arrived_ref[owner, rows + cut :, :]
    piece_ref[...] = piece
    for p in range(n):
        sent_ref[p, 0:rows, :] = piece
        sent_ref[p, rows:, :] = strip
    small_ref[0:cut] = total[rows:]
    small_ref[cut : cut + thin] = piece_ref[pl.ds(pl.multiple_of(sub * thin, thin), thin), :]
    small_ref[cut + thin :] = arrived_ref[
        owner,
        pl.ds(pl.multiple_of(rows + cut + 2 * sub * thin, 8), 2 * thin),
        :,
    ]


def third_kernel(block_ref, gathered_ref, sent_ref, *, groups):
    n, small, _ = gathered_ref.shape
    cut = L // n
    owner, _ = place_of(block_ref, groups)
    total = gathered_ref[0, 0:cut, :]
    for p in range(1, n):
        total = total + gathered_ref[p, 0:cut, :]
    sent_ref[0:cut] = total
    sent_ref[cut:] = gathered_ref[owner, cut:small, :]


def pack_kernel(window_ref, turned_ref, sent_ref):
    lines = window_ref.shape[0]
    window = window_ref[...]
    turned = turned_ref[...]
    first = turned.astype(BF16)
    second = (turned - first.astype(F32)).astype(BF16)
    for p in range(sent_ref.shape[0]):
        sent_ref[p, 0:lines, :] = window
        sent_ref[p, lines:, 0:L] = first
        sent_ref[p, lines:, L:] = second


def last_kernel(
    h_ref, w_ref, own_ref, other_ref, twice_ref, low_ref, comp_ref, updated_ref, pruned_ref,
    right_ref, window_ref,
):
    count, lines, _ = own_ref.shape
    step = pl.program_id(0)
    tile = right_ref.shape[0]
    thin = B // (2 * count)
    groups = tile // B
    lines -= groups * thin

    @pl.when(step == 0)
    def _():
        core = lax.axis_index("core")
        for ref, c in ((own_ref, core), (other_ref, 1 - core)):
            for z in range(count):
                window_ref[c * count + z] = ref[z, 0:lines, :]
                for s in range(groups):
                    at = s * B + (2 * z + c) * thin
                    right_ref[pl.ds(pl.multiple_of(at, thin), thin), :] = ref[
                        z, lines + s * thin : lines + (s + 1) * thin, :
                    ]

    part = h_ref.shape[0]
    right = right_ref[pl.ds(pl.multiple_of(step * part, 16), part), :]
    dims = (((1,), (1,)), ((), ()))
    change = lax.dot_general(right, twice_ref[...], dims, preferred_element_type=F32)
    change += lax.dot_general(right[:, :L], low_ref[...], dims, preferred_element_type=F32)
    updated_ref[...] = h_ref[...] - change
    some = w_ref.shape[0] // lines
    comp = comp_ref[...]
    for q in range(some):
        window = window_ref[step * some + q]
        product = jnp.dot(window, comp, preferred_element_type=F32)
        pruned_ref[q * lines : (q + 1) * lines, :] = (
            w_ref[q * lines : (q + 1) * lines, :].astype(F32) - product
        ).astype(BF16)


def invert(a_ref):
    lane = lax.broadcasted_iota(jnp.int32, (8, L), 1)
    sub = lax.broadcasted_iota(jnp.int32, (8, L), 0)
    wide_lane = lax.broadcasted_iota(jnp.int32, (L, L), 1)

    def step(k, carry):
        base = pl.multiple_of(8 * k, 8)
        panel = a_ref[pl.ds(base, 8), :]
        columns = [
            jnp.broadcast_to(
                jnp.sum(jnp.where(lane == base + j, panel, 0.0), axis=1, keepdims=True), (8, L)
            )
            for j in range(8)
        ]
        whole = a_ref[...]
        factors = [
            jnp.sum(jnp.where(wide_lane == base + j, whole, 0.0), axis=1, keepdims=True)
            for j in range(8)
        ]
        for j in range(8):
            own = columns[j]
            inverse = 1.0 / own[j : j + 1, :]
            here = sub == j
            panel = jnp.where(lane == base + j, jnp.where(here, 1.0, 0.0), panel)
            scaled = panel[j : j + 1, :] * inverse
            panel = jnp.where(here, scaled, panel - own * scaled)
            for m in range(j + 1, 8):
                scaled = columns[m][j : j + 1, :] * inverse
                columns[m] = jnp.where(here, scaled, columns[m] - own * scaled)
        inside = (wide_lane >= base) & (wide_lane < base + 8)
        rest = jnp.where(inside, 0.0, whole)
        for j in range(8):
            rest = rest - factors[j] * panel[j : j + 1, :]
        a_ref[...] = rest
        a_ref[pl.ds(base, 8), :] = panel
        return carry

    lax.fori_loop(0, L // 8, step, 0)


def fourth_kernel(
    c_ref, large_ref, twice_ref, low_ref, comp_ref, a_ref, gm_ref, gc_ref, q_ref, st_ref
):
    n = c_ref.shape[0]
    tile = gc_ref.shape[0]
    thin, cut, groups, wide = B // n, L // n, tile // B, tile // L
    for p in range(n):
        a_ref[p * cut : (p + 1) * cut, :] = c_ref[p, 0:cut, :]
        at = cut
        gm_ref[p * thin : (p + 1) * thin, :] = c_ref[p, at : at + thin, :]
        at += thin
        for w in range(2):
            q_ref[p * thin : (p + 1) * thin, w * L : (w + 1) * L] = c_ref[p, at : at + thin, :]
            at += thin
        at = 0
        for s in range(groups):
            gc_ref[s * B + p * thin : s * B + (p + 1) * thin, :] = large_ref[p, at : at + thin, :]
            at += thin
        for w in range(wide):
            st_ref[p * thin : (p + 1) * thin, w * L : (w + 1) * L] = large_ref[
                p, at : at + thin, :
            ]
            at += thin
    inner = a_ref[...]
    same = lax.broadcasted_iota(jnp.int32, (L, L), 0) == lax.broadcasted_iota(
        jnp.int32, (L, L), 1
    )
    a_ref[...] = jnp.where(same, 1.0, 0.0) + 0.5 * (inner + inner.T)
    invert(a_ref)
    x = a_ref[...]
    block_right = gm_ref[...]
    right = gc_ref[...]
    half = dot(block_right, x)
    solved = dot(right, x)
    high = solved.astype(BF16)
    twice_ref[:, 0:L] = high
    twice_ref[:, L:] = high
    low_ref[...] = (solved - high.astype(F32)).astype(BF16)
    square = q_ref[...] - dot_nt(half, block_right)
    square = 0.5 * (square + square.T)
    a_ref[...] = square[:L, :L]
    st_ref[...] = st_ref[...] - dot_nt(half, right)
    invert(a_ref)
    u = a_ref[...]
    v = dot(square[L:, :L], u)
    a_ref[...] = square[L:, L:] - dot(v, square[:L, L:])
    top = st_ref[0:L, :]
    first = dot(u, top)
    second = st_ref[L:, :] - dot(v, top)
    invert(a_ref)
    second = dot(a_ref[...], second)
    comp_ref[0:L, :] = (first - dot(v.T, second)).astype(BF16)
    comp_ref[L:, :] = second.astype(BF16)


VMEM = pl.BlockSpec(memory_space=pltpu.VMEM)
PARAMS = pltpu.CompilerParams(vmem_limit_bytes=10 * 2**20)
FIRST_PARAMS = pltpu.CompilerParams(vmem_limit_bytes=58 * 2**20)
SMEM = pl.BlockSpec(memory_space=pltpu.SMEM)
HBM = pl.BlockSpec(memory_space=pltpu.HBM)


def of(shape, dtype=F32):
    return jax.ShapeDtypeStruct(shape, dtype)


def all_steps(inv_hessian, weights, calib, block):
    tile = inv_hessian.shape[0]
    n = lax.axis_size(ROW)
    count = lax.axis_size("z")
    lines = weights.shape[0] // n
    thin, cut, groups, wide = B // n, L // n, tile // B, tile // L
    rows = groups * thin
    strip_rows = wide * thin
    small_rows = cut + 3 * thin
    sent, keep, give = pl.pallas_call(
        first_kernel,
        out_shape=(
            of((n, rows + cut + strip_rows, L)),
            of((count, lines, B), BF16),
            of((count, lines, B), BF16),
        ),
        in_specs=[SMEM, VMEM, HBM, HBM],
        out_specs=(VMEM, VMEM, VMEM),
        scratch_shapes=[
            pltpu.VMEM((L, tile), BF16),
            pltpu.VMEM((L, tile), BF16),
            pltpu.SemaphoreType.DMA((4,)),
        ],
        compiler_params=FIRST_PARAMS,
        name="first",
    )(block, inv_hessian, calib, weights.reshape(n, lines, tile))
    arrived = exchanged(sent, ROW)
    got = lax.ppermute(give, "core", [(0, 1), (1, 0)])
    turned = pl.pallas_call(
        partial(choose_kernel, groups=groups),
        out_shape=(of((lines, B), BF16),) * count,
        in_specs=[SMEM, VMEM, VMEM],
        out_specs=(VMEM,) * count,
        compiler_params=PARAMS,
        name="choose",
    )(block, keep, got)
    shifted = [turned[0]]
    for k in range(1, count):
        perm = [(i, (i + k) % count) for i in range(count)]
        shifted.append(lax.ppermute(turned[k], "z", perm))
    small, piece, large, window = pl.pallas_call(
        second_kernel,
        out_shape=(
            of((small_rows, L)),
            of((rows, L)),
            of((n, rows + strip_rows, L)),
            of((lines, B), BF16),
        ),
        in_specs=[SMEM] + [VMEM] * (1 + count),
        out_specs=(VMEM, VMEM, VMEM, VMEM),
        compiler_params=PARAMS,
        name="second",
    )(block, arrived, *shifted)
    turn = [(i * n + j, j * n + i) for i in range(n) for j in range(n)]
    turned = lax.ppermute(piece, (*ROW, *COL), turn)
    large = exchanged(large, ROW)
    gathered = lax.all_gather(small, "core")
    gathered = lax.all_gather(gathered, "z").reshape(n, small_rows, L)
    sent = pl.pallas_call(
        partial(third_kernel, groups=groups),
        out_shape=of((small_rows, L)),
        in_specs=[SMEM, VMEM],
        out_specs=VMEM,
        compiler_params=PARAMS,
        name="third",
    )(block, gathered)
    arrived = lax.all_gather(sent, "y")
    arrived = lax.all_gather(arrived, "x").reshape(n, small_rows, L)
    packed = pl.pallas_call(
        pack_kernel,
        out_shape=of((count, lines + rows, B), BF16),
        in_specs=[VMEM, VMEM],
        out_specs=VMEM,
        compiler_params=PARAMS,
        name="pack",
    )(window, turned)
    packed = exchanged(packed, "z")
    other = lax.ppermute(packed, "core", [(0, 1), (1, 0)])
    twice, low, comp = pl.pallas_call(
        fourth_kernel,
        out_shape=(of((tile, 2 * L), BF16), of((tile, L), BF16), of((B, tile), BF16)),
        in_specs=[VMEM, VMEM],
        out_specs=(VMEM, VMEM, VMEM),
        scratch_shapes=[
            pltpu.VMEM((L, L), F32),
            pltpu.VMEM((B, L), F32),
            pltpu.VMEM((tile, L), F32),
            pltpu.VMEM((B, B), F32),
            pltpu.VMEM((B, tile), F32),
        ],
        cost_estimate=pl.CostEstimate(
            flops=20_000_000_000, bytes_accessed=4_000_000, transcendentals=0
        ),
        compiler_params=PARAMS,
        name="fourth",
    )(arrived, large)
    steps = 4
    return pl.pallas_call(
        last_kernel,
        grid=(steps,),
        out_shape=(of((tile, tile)), of((n * lines, tile), BF16)),
        in_specs=[
            pl.BlockSpec((tile // steps, tile), lambda i: (i, 0)),
            pl.BlockSpec((n * lines // steps, tile), lambda i: (i, 0)),
            VMEM,
            VMEM,
            VMEM,
            VMEM,
            VMEM,
        ],
        out_specs=(
            pl.BlockSpec((tile // steps, tile), lambda i: (i, 0)),
            pl.BlockSpec((n * lines // steps, tile), lambda i: (i, 0)),
        ),
        scratch_shapes=[pltpu.VMEM((tile, 2 * L), BF16), pltpu.VMEM((n, lines, B), BF16)],
        compiler_params=PARAMS,
        name="last",
    )(inv_hessian, weights, packed, other, twice, low, comp)


def solution(mesh):
    finer = Mesh(mesh.devices.reshape(4, 4, 8, 2), (*ROW, *COL))
    specs = (P(ROW, COL), P(ROW, COL), P(), P())
    return jax.shard_map(
        all_steps, mesh=finer, in_specs=specs, out_specs=specs[:2], check_vma=False
    )
```

```python
from functools import partial

import jax
import jax.numpy as jnp
from jax import lax
from jax.experimental import pallas as pl
from jax.experimental.pallas import tpu as pltpu
from jax.sharding import Mesh
from jax.sharding import PartitionSpec as P

B = 256
L = 128
ROW = ("x", "y")
COL = ("z", "core")
F32 = jnp.float32
BF16 = jnp.bfloat16
HIGHEST = lax.Precision.HIGHEST


def exchanged(parts, axis):
    return lax.all_to_all(parts, axis, split_axis=0, concat_axis=0, tiled=True)


def dot(a, b, dims=((1,), (0,))):
    return lax.dot_general(a, b, (dims, ((), ())), precision=HIGHEST, preferred_element_type=F32)


def dot_nt(a, b):
    return dot(a, b, ((1,), (1,)))


def in_three(x):
    first = x.astype(BF16)
    rest = x - first.astype(F32)
    second = rest.astype(BF16)
    third = (rest - second.astype(F32)).astype(BF16)
    return first, second, third


def place_of(block_ref, groups):
    owner = block_ref[0] // groups
    return owner, block_ref[0] - owner * groups


def first_kernel(
    block_ref, h_ref, calib_ref, w_ref, sent_ref, keep_ref, give_ref, rows_ref, cols_ref, sems
):
    n = sent_ref.shape[0]
    half = keep_ref.shape[0]
    tile = h_ref.shape[1]
    groups, wide, thin = tile // B, tile // L, B // n
    _, sub = place_of(block_ref, groups)
    row = lax.axis_index("x") * lax.axis_size("y") + lax.axis_index("y")
    core = lax.axis_index("core")
    col = lax.axis_index("z") * lax.axis_size("core") + core
    offset = pl.multiple_of(sub * B, B)

    def window_of(which):
        return w_ref.at[pl.ds(which * half, half), :, pl.ds(offset, B)]

    copies = [
        pltpu.make_async_copy(
            calib_ref.at[:, pl.ds(pl.multiple_of(row * tile, L), tile)], rows_ref, sems.at[0]
        ),
        pltpu.make_async_copy(
            calib_ref.at[:, pl.ds(pl.multiple_of(col * tile, L), tile)], cols_ref, sems.at[1]
        ),
        pltpu.make_async_copy(window_of(core), keep_ref, sems.at[2]),
        pltpu.make_async_copy(window_of(1 - core), give_ref, sems.at[3]),
    ]
    for copy in copies:
        copy.start()
    copies[0].wait()
    copies[1].wait()
    first, second, third = in_three(h_ref[...])
    rows = rows_ref[...]
    left = jnp.dot(rows, first, preferred_element_type=F32)
    left += jnp.dot(rows, second, preferred_element_type=F32)
    left += jnp.dot(rows, third, preferred_element_type=F32)
    right = left.T
    cols = cols_ref[...]
    dims = (((1,), (1,)), ((), ()))
    first, second, third = in_three(left)
    inner = lax.dot_general(first, cols, dims, preferred_element_type=F32)
    inner += lax.dot_general(second, cols, dims, preferred_element_type=F32)
    inner += lax.dot_general(third, cols, dims, preferred_element_type=F32)
    cut = L // n
    for p in range(n):
        for s in range(groups):
            at = s * B + p * thin
            sent_ref[p, s * thin : (s + 1) * thin, :] = right[at : at + thin]
        at = groups * thin
        sent_ref[p, at : at + cut, :] = inner[p * cut : (p + 1) * cut]
        at += cut
        for w in range(wide):
            sent_ref[p, at + w * thin : at + (w + 1) * thin, :] = h_ref[
                pl.ds(pl.multiple_of(offset + p * thin, thin), thin), w * L : (w + 1) * L
            ]
    copies[2].wait()
    copies[3].wait()


def choose_kernel(block_ref, keep_ref, got_ref, *turned_refs, groups):
    count = len(turned_refs)
    owner, _ = place_of(block_ref, groups)
    z = lax.axis_index("z")
    own = owner % 2 == lax.axis_index("core")
    for k in range(count):
        at = (z + k) % count
        turned_refs[k][...] = jnp.where(own, keep_ref[at], got_ref[at])


def pick_shifted(block_ref, shifted, window_ref, groups, count, first=0):
    owner, _ = place_of(block_ref, groups)
    away = (lax.axis_index("z") + count - owner // 2) % count
    for k, ref in enumerate(shifted):

        @pl.when(away == first + k)
        def _(ref=ref):
            window_ref[...] = ref[...]


def second_kernel(block_ref, arrived_ref, *refs, count):
    *shifted, small_ref, piece_ref, strip_ref, window_ref = refs
    n = arrived_ref.shape[0]
    rows = piece_ref.shape[0]
    thin, cut = B // n, L // n
    owner, sub = place_of(block_ref, rows // thin)
    pick_shifted(block_ref, shifted, window_ref, rows // thin, count)
    total = arrived_ref[0, 0 : rows + cut, :]
    for p in range(1, n):
        total = total + arrived_ref[p, 0 : rows + cut, :]
    piece_ref[...] = total[:rows]
    strip_ref[...] = arrived_ref[owner, rows + cut :, :]
    small_ref[0:cut] = total[rows:]
    small_ref[cut : cut + thin] = piece_ref[pl.ds(pl.multiple_of(sub * thin, thin), thin), :]
    small_ref[cut + thin :] = strip_ref[
        pl.ds(pl.multiple_of(2 * sub * thin, 2 * thin), 2 * thin), :
    ]


def third_kernel(block_ref, gathered_ref, piece_ref, strip_ref, sent_ref):
    n, small, _ = gathered_ref.shape
    rows = piece_ref.shape[0]
    cut = L // n
    owner, _ = place_of(block_ref, rows * n // B)
    total = gathered_ref[0, 0:cut, :]
    for p in range(1, n):
        total = total + gathered_ref[p, 0:cut, :]
    chosen = gathered_ref[owner, cut:small, :]
    piece, strip = piece_ref[...], strip_ref[...]
    for p in range(n):
        sent_ref[p, 0:cut, :] = total
        sent_ref[p, cut:small, :] = chosen
        sent_ref[p, small : small + rows, :] = piece
        sent_ref[p, small + rows :, :] = strip


def pack_kernel(block_ref, window_ref, turned_ref, *refs, groups):
    *shifted, sent_ref, chosen_ref = refs
    lines = window_ref.shape[0]
    count = sent_ref.shape[0]
    chosen_ref[...] = window_ref[...]
    pick_shifted(block_ref, shifted, chosen_ref, groups, count, count - len(shifted))
    window = chosen_ref[...]
    turned = turned_ref[...]
    first = turned.astype(BF16)
    second = (turned - first.astype(F32)).astype(BF16)
    for p in range(count):
        sent_ref[p, 0:lines, :] = window
        sent_ref[p, lines:, 0:L] = first
        sent_ref[p, lines:, L:] = second


def last_kernel(
    h_ref, w_ref, own_ref, other_ref, twice_ref, low_ref, comp_ref, updated_ref, pruned_ref,
    right_ref, window_ref,
):
    count, lines, _ = own_ref.shape
    step = pl.program_id(0)
    tile = right_ref.shape[0]
    thin = B // (2 * count)
    groups = tile // B
    lines -= groups * thin

    @pl.when(step == 0)
    def _():
        core = lax.axis_index("core")
        for ref, c in ((own_ref, core), (other_ref, 1 - core)):
            for z in range(count):
                window_ref[c * count + z] = ref[z, 0:lines, :]
                for s in range(groups):
                    at = s * B + (2 * z + c) * thin
                    right_ref[pl.ds(pl.multiple_of(at, thin), thin), :] = ref[
                        z, lines + s * thin : lines + (s + 1) * thin, :
                    ]

    part = h_ref.shape[0]
    right = right_ref[pl.ds(pl.multiple_of(step * part, 16), part), :]
    dims = (((1,), (1,)), ((), ()))
    change = lax.dot_general(right, twice_ref[...], dims, preferred_element_type=F32)
    change += lax.dot_general(right[:, :L], low_ref[...], dims, preferred_element_type=F32)
    updated_ref[...] = h_ref[...] - change
    some = w_ref.shape[0] // lines
    comp = comp_ref[...]
    for q in range(some):
        window = window_ref[step * some + q]
        product = jnp.dot(window, comp, preferred_element_type=F32)
        pruned_ref[q * lines : (q + 1) * lines, :] = (
            w_ref[q * lines : (q + 1) * lines, :].astype(F32) - product
        ).astype(BF16)


def invert(a_ref):
    lane = lax.broadcasted_iota(jnp.int32, (8, L), 1)
    sub = lax.broadcasted_iota(jnp.int32, (8, L), 0)
    wide_lane = lax.broadcasted_iota(jnp.int32, (L, L), 1)

    def step(k, carry):
        base = pl.multiple_of(8 * k, 8)
        panel = a_ref[pl.ds(base, 8), :]
        columns = [
            jnp.broadcast_to(
                jnp.sum(jnp.where(lane == base + j, panel, 0.0), axis=1, keepdims=True), (8, L)
            )
            for j in range(8)
        ]
        whole = a_ref[...]
        factors = [
            jnp.sum(jnp.where(wide_lane == base + j, whole, 0.0), axis=1, keepdims=True)
            for j in range(8)
        ]
        for j in range(8):
            own = columns[j]
            inverse = 1.0 / own[j : j + 1, :]
            here = sub == j
            panel = jnp.where(lane == base + j, jnp.where(here, 1.0, 0.0), panel)
            scaled = panel[j : j + 1, :] * inverse
            panel = jnp.where(here, scaled, panel - own * scaled)
            for m in range(j + 1, 8):
                scaled = columns[m][j : j + 1, :] * inverse
                columns[m] = jnp.where(here, scaled, columns[m] - own * scaled)
        inside = (wide_lane >= base) & (wide_lane < base + 8)
        rest = jnp.where(inside, 0.0, whole)
        for j in range(8):
            rest = rest - factors[j] * panel[j : j + 1, :]
        a_ref[...] = rest
        a_ref[pl.ds(base, 8), :] = panel
        return carry

    lax.fori_loop(0, L // 8, step, 0)


def fourth_kernel(
    c_ref, twice_ref, low_ref, comp_ref, a_ref, gm_ref, gc_ref, q_ref, st_ref
):
    n = c_ref.shape[0]
    tile = gc_ref.shape[0]
    thin, cut, groups, wide = B // n, L // n, tile // B, tile // L
    for p in range(n):
        a_ref[p * cut : (p + 1) * cut, :] = c_ref[p, 0:cut, :]
        at = cut
        gm_ref[p * thin : (p + 1) * thin, :] = c_ref[p, at : at + thin, :]
        at += thin
        for w in range(2):
            q_ref[p * thin : (p + 1) * thin, w * L : (w + 1) * L] = c_ref[p, at : at + thin, :]
            at += thin
        for s in range(groups):
            gc_ref[s * B + p * thin : s * B + (p + 1) * thin, :] = c_ref[p, at : at + thin, :]
            at += thin
        for w in range(wide):
            st_ref[p * thin : (p + 1) * thin, w * L : (w + 1) * L] = c_ref[p, at : at + thin, :]
            at += thin
    inner = a_ref[...]
    same = lax.broadcasted_iota(jnp.int32, (L, L), 0) == lax.broadcasted_iota(
        jnp.int32, (L, L), 1
    )
    a_ref[...] = jnp.where(same, 1.0, 0.0) + 0.5 * (inner + inner.T)
    invert(a_ref)
    x = a_ref[...]
    block_right = gm_ref[...]
    right = gc_ref[...]
    half = dot(block_right, x)
    solved = dot(right, x)
    high = solved.astype(BF16)
    twice_ref[:, 0:L] = high
    twice_ref[:, L:] = high
    low_ref[...] = (solved - high.astype(F32)).astype(BF16)
    square = q_ref[...] - dot_nt(half, block_right)
    square = 0.5 * (square + square.T)
    a_ref[...] = square[:L, :L]
    st_ref[...] = st_ref[...] - dot_nt(half, right)
    invert(a_ref)
    u = a_ref[...]
    v = dot(square[L:, :L], u)
    a_ref[...] = square[L:, L:] - dot(v, square[:L, L:])
    top = st_ref[0:L, :]
    first = dot(u, top)
    second = st_ref[L:, :] - dot(v, top)
    invert(a_ref)
    second = dot(a_ref[...], second)
    comp_ref[0:L, :] = (first - dot(v.T, second)).astype(BF16)
    comp_ref[L:, :] = second.astype(BF16)


VMEM = pl.BlockSpec(memory_space=pltpu.VMEM)
PARAMS = pltpu.CompilerParams(vmem_limit_bytes=10 * 2**20)
FIRST_PARAMS = pltpu.CompilerParams(vmem_limit_bytes=58 * 2**20)
LAST_PARAMS = pltpu.CompilerParams(vmem_limit_bytes=51 * 2**20)
SMEM = pl.BlockSpec(memory_space=pltpu.SMEM)
HBM = pl.BlockSpec(memory_space=pltpu.HBM)


def of(shape, dtype=F32):
    return jax.ShapeDtypeStruct(shape, dtype)


def all_steps(inv_hessian, weights, calib, block):
    tile = inv_hessian.shape[0]
    n = lax.axis_size(ROW)
    count = lax.axis_size("z")
    lines = weights.shape[0] // n
    thin, cut, groups, wide = B // n, L // n, tile // B, tile // L
    rows = groups * thin
    strip_rows = wide * thin
    small_rows = cut + 3 * thin
    sent, keep, give = pl.pallas_call(
        first_kernel,
        out_shape=(
            of((n, rows + cut + strip_rows, L)),
            of((count, lines, B), BF16),
            of((count, lines, B), BF16),
        ),
        in_specs=[SMEM, VMEM, HBM, HBM],
        out_specs=(VMEM, VMEM, VMEM),
        scratch_shapes=[
            pltpu.VMEM((L, tile), BF16),
            pltpu.VMEM((L, tile), BF16),
            pltpu.SemaphoreType.DMA((4,)),
        ],
        compiler_params=FIRST_PARAMS,
        name="first",
    )(block, inv_hessian, calib, weights.reshape(n, lines, tile))
    arrived = exchanged(sent, ROW)
    got = lax.ppermute(give, "core", [(0, 1), (1, 0)])
    turned = pl.pallas_call(
        partial(choose_kernel, groups=groups),
        out_shape=(of((lines, B), BF16),) * count,
        in_specs=[SMEM, VMEM, VMEM],
        out_specs=(VMEM,) * count,
        compiler_params=PARAMS,
        name="choose",
    )(block, keep, got)
    early = count // 2 + 1
    shifted = [turned[0]]
    for k in range(1, count):
        perm = [(i, (i + k) % count) for i in range(count)]
        shifted.append(lax.ppermute(turned[k], "z", perm))
    small, piece, strip, window = pl.pallas_call(
        partial(second_kernel, count=count),
        out_shape=(
            of((small_rows, L)),
            of((rows, L)),
            of((strip_rows, L)),
            of((lines, B), BF16),
        ),
        in_specs=[SMEM] + [VMEM] * (1 + early),
        out_specs=(VMEM, VMEM, VMEM, VMEM),
        compiler_params=PARAMS,
        name="second",
    )(block, arrived, *shifted[:early])
    turn = [(i * n + j, j * n + i) for i in range(n) for j in range(n)]
    turned = lax.ppermute(piece, (*ROW, *COL), turn)
    gathered = lax.all_gather(small, "core")
    gathered = lax.all_gather(gathered, "z").reshape(n, small_rows, L)
    sent = pl.pallas_call(
        third_kernel,
        out_shape=of((n, small_rows + rows + strip_rows, L)),
        in_specs=[SMEM, VMEM, VMEM, VMEM],
        out_specs=VMEM,
        compiler_params=PARAMS,
        name="third",
    )(block, gathered, piece, strip)
    arrived = exchanged(sent, ROW)
    packed = pl.pallas_call(
        partial(pack_kernel, groups=groups),
        out_shape=of((count, lines + rows, B), BF16),
        in_specs=[SMEM] + [VMEM] * (2 + count - early),
        out_specs=VMEM,
        scratch_shapes=[pltpu.VMEM((lines, B), BF16)],
        compiler_params=PARAMS,
        name="pack",
    )(block, window, turned, *shifted[early:])
    packed = exchanged(packed, "z")
    other = lax.ppermute(packed, "core", [(0, 1), (1, 0)])
    twice, low, comp = pl.pallas_call(
        fourth_kernel,
        out_shape=(of((tile, 2 * L), BF16), of((tile, L), BF16), of((B, tile), BF16)),
        in_specs=[VMEM],
        out_specs=(VMEM, VMEM, VMEM),
        scratch_shapes=[
            pltpu.VMEM((L, L), F32),
            pltpu.VMEM((B, L), F32),
            pltpu.VMEM((tile, L), F32),
            pltpu.VMEM((B, B), F32),
            pltpu.VMEM((B, tile), F32),
        ],
        cost_estimate=pl.CostEstimate(
            flops=20_000_000_000, bytes_accessed=4_000_000, transcendentals=0
        ),
        compiler_params=PARAMS,
        name="fourth",
    )(arrived)
    steps = 4
    return pl.pallas_call(
        last_kernel,
        grid=(steps,),
        out_shape=(of((tile, tile)), of((n * lines, tile), BF16)),
        in_specs=[
            pl.BlockSpec((tile // steps, tile), lambda i: (i, 0)),
            pl.BlockSpec((n * lines // steps, tile), lambda i: (i, 0)),
            VMEM,
            VMEM,
            VMEM,
            VMEM,
            VMEM,
        ],
        out_specs=(
            pl.BlockSpec((tile // steps, tile), lambda i: (i, 0)),
            pl.BlockSpec((n * lines // steps, tile), lambda i: (i, 0)),
        ),
        scratch_shapes=[pltpu.VMEM((tile, 2 * L), BF16), pltpu.VMEM((n, lines, B), BF16)],
        compiler_params=LAST_PARAMS,
        name="last",
    )(inv_hessian, weights, packed, other, twice, low, comp)


def solution(mesh):
    finer = Mesh(mesh.devices.reshape(4, 4, 8, 2), (*ROW, *COL))
    specs = (P(ROW, COL), P(ROW, COL), P(), P())
    return jax.shard_map(
        all_steps, mesh=finer, in_specs=specs, out_specs=specs[:2], check_vma=False
    )
```

```python
from functools import partial

import jax
import jax.numpy as jnp
from jax import lax
from jax.experimental import pallas as pl
from jax.experimental.pallas import tpu as pltpu
from jax.sharding import Mesh
from jax.sharding import PartitionSpec as P

B = 256
L = 128
ROW = ("x", "y")
COL = ("z", "core")
F32 = jnp.float32
BF16 = jnp.bfloat16
HIGHEST = lax.Precision.HIGHEST


def exchanged(parts, axis):
    return lax.all_to_all(parts, axis, split_axis=0, concat_axis=0, tiled=True)


def dot(a, b, dims=((1,), (0,))):
    return lax.dot_general(a, b, (dims, ((), ())), precision=HIGHEST, preferred_element_type=F32)


def dot_nt(a, b):
    return dot(a, b, ((1,), (1,)))


def in_three(x):
    first = x.astype(BF16)
    rest = x - first.astype(F32)
    second = rest.astype(BF16)
    third = (rest - second.astype(F32)).astype(BF16)
    return first, second, third


def place_of(block_ref, groups):
    owner = block_ref[0] // groups
    return owner, block_ref[0] - owner * groups


def first_kernel(
    block_ref, source_ref, calib_ref, w_ref, sent_ref, keep_ref, give_ref,
    h_ref, rows_ref, cols_ref, sems,
):
    n = sent_ref.shape[0]
    half = keep_ref.shape[0]
    tile = h_ref.shape[1]
    groups, wide, thin = tile // B, tile // L, B // n
    _, sub = place_of(block_ref, groups)
    row = lax.axis_index("x") * lax.axis_size("y") + lax.axis_index("y")
    core = lax.axis_index("core")
    col = lax.axis_index("z") * lax.axis_size("core") + core
    offset = pl.multiple_of(sub * B, B)

    def window_of(which):
        return w_ref.at[pl.ds(which * half, half), :, pl.ds(offset, B)]

    copies = [
        pltpu.make_async_copy(
            calib_ref.at[:, pl.ds(pl.multiple_of(row * tile, L), tile)], rows_ref, sems.at[0]
        ),
        pltpu.make_async_copy(
            calib_ref.at[:, pl.ds(pl.multiple_of(col * tile, L), tile)], cols_ref, sems.at[1]
        ),
        pltpu.make_async_copy(window_of(core), keep_ref, sems.at[2]),
        pltpu.make_async_copy(window_of(1 - core), give_ref, sems.at[3]),
    ]
    blocks = [
        pltpu.make_async_copy(
            source_ref.at[g * B : (g + 1) * B, :], h_ref.at[g * B : (g + 1) * B, :], sems.at[4 + g]
        )
        for g in range(groups)
    ]
    copies[0].start()
    blocks[0].start()
    copies[1].start()
    for copy in blocks[1:] + copies[2:]:
        copy.start()
    copies[0].wait()
    left = None
    for g in range(groups):
        blocks[g].wait()
        rows = rows_ref[:, g * B : (g + 1) * B]
        for part in in_three(h_ref[g * B : (g + 1) * B, :]):
            more = jnp.dot(rows, part, preferred_element_type=F32)
            left = more if left is None else left + more
    copies[1].wait()
    right = left.T
    cols = cols_ref[...]
    dims = (((1,), (1,)), ((), ()))
    first, second, third = in_three(left)
    inner = lax.dot_general(first, cols, dims, preferred_element_type=F32)
    inner += lax.dot_general(second, cols, dims, preferred_element_type=F32)
    inner += lax.dot_general(third, cols, dims, preferred_element_type=F32)
    cut = L // n
    for p in range(n):
        for s in range(groups):
            at = s * B + p * thin
            sent_ref[p, s * thin : (s + 1) * thin, :] = right[at : at + thin]
        at = groups * thin
        sent_ref[p, at : at + cut, :] = inner[p * cut : (p + 1) * cut]
        at += cut
        for w in range(wide):
            sent_ref[p, at + w * thin : at + (w + 1) * thin, :] = h_ref[
                pl.ds(pl.multiple_of(offset + p * thin, thin), thin), w * L : (w + 1) * L
            ]
    copies[2].wait()
    copies[3].wait()


def choose_kernel(block_ref, keep_ref, got_ref, *turned_refs, groups):
    count = len(turned_refs)
    owner, _ = place_of(block_ref, groups)
    z = lax.axis_index("z")
    own = owner % 2 == lax.axis_index("core")
    for k in range(count):
        at = (z + k) % count
        turned_refs[k][...] = jnp.where(own, keep_ref[at], got_ref[at])


def pick_shifted(block_ref, shifted, window_ref, groups, count, first=0):
    owner, _ = place_of(block_ref, groups)
    away = (lax.axis_index("z") + count - owner // 2) % count
    for k, ref in enumerate(shifted):

        @pl.when(away == first + k)
        def _(ref=ref):
            window_ref[...] = ref[...]


def second_kernel(block_ref, arrived_ref, *refs, count):
    *shifted, small_ref, piece_ref, strip_ref, window_ref = refs
    n = arrived_ref.shape[0]
    rows = piece_ref.shape[0]
    thin, cut = B // n, L // n
    owner, sub = place_of(block_ref, rows // thin)
    pick_shifted(block_ref, shifted, window_ref, rows // thin, count)
    total = arrived_ref[0, 0 : rows + cut, :]
    for p in range(1, n):
        total = total + arrived_ref[p, 0 : rows + cut, :]
    piece_ref[...] = total[:rows]
    strip_ref[...] = arrived_ref[owner, rows + cut :, :]
    small_ref[0:cut] = total[rows:]
    small_ref[cut : cut + thin] = piece_ref[pl.ds(pl.multiple_of(sub * thin, thin), thin), :]
    small_ref[cut + thin :] = strip_ref[
        pl.ds(pl.multiple_of(2 * sub * thin, 2 * thin), 2 * thin), :
    ]


def third_kernel(block_ref, gathered_ref, piece_ref, strip_ref, sent_ref):
    n, small, _ = gathered_ref.shape
    rows = piece_ref.shape[0]
    cut = L // n
    owner, _ = place_of(block_ref, rows * n // B)
    total = gathered_ref[0, 0:cut, :]
    for p in range(1, n):
        total = total + gathered_ref[p, 0:cut, :]
    chosen = gathered_ref[owner, cut:small, :]
    piece, strip = piece_ref[...], strip_ref[...]
    for p in range(n):
        sent_ref[p, 0:cut, :] = total
        sent_ref[p, cut:small, :] = chosen
        sent_ref[p, small : small + rows, :] = piece
        sent_ref[p, small + rows :, :] = strip


def pack_kernel(block_ref, window_ref, turned_ref, *refs, groups):
    *shifted, sent_ref, chosen_ref = refs
    lines = window_ref.shape[0]
    count = sent_ref.shape[0]
    chosen_ref[...] = window_ref[...]
    pick_shifted(block_ref, shifted, chosen_ref, groups, count, count - len(shifted))
    window = chosen_ref[...]
    turned = turned_ref[...]
    first = turned.astype(BF16)
    second = (turned - first.astype(F32)).astype(BF16)
    for p in range(count):
        sent_ref[p, 0:lines, :] = window
        sent_ref[p, lines:, 0:L] = first
        sent_ref[p, lines:, L:] = second


def last_kernel(
    h_ref, w_ref, own_ref, other_ref, twice_ref, low_ref, comp_ref, updated_ref, pruned_ref,
    right_ref, window_ref,
):
    count, lines, _ = own_ref.shape
    step = pl.program_id(0)
    tile = right_ref.shape[0]
    thin = B // (2 * count)
    groups = tile // B
    lines -= groups * thin

    @pl.when(step == 0)
    def _():
        core = lax.axis_index("core")
        for ref, c in ((own_ref, core), (other_ref, 1 - core)):
            for z in range(count):
                window_ref[c * count + z] = ref[z, 0:lines, :]
                for s in range(groups):
                    at = s * B + (2 * z + c) * thin
                    right_ref[pl.ds(pl.multiple_of(at, thin), thin), :] = ref[
                        z, lines + s * thin : lines + (s + 1) * thin, :
                    ]

    part = h_ref.shape[0]
    right = right_ref[pl.ds(pl.multiple_of(step * part, 16), part), :]
    dims = (((1,), (1,)), ((), ()))
    change = lax.dot_general(right, twice_ref[...], dims, preferred_element_type=F32)
    change += lax.dot_general(right[:, :L], low_ref[...], dims, preferred_element_type=F32)
    updated_ref[...] = h_ref[...] - change
    some = w_ref.shape[0] // lines
    comp = comp_ref[...]
    for q in range(some):
        window = window_ref[step * some + q]
        product = jnp.dot(window, comp, preferred_element_type=F32)
        pruned_ref[q * lines : (q + 1) * lines, :] = (
            w_ref[q * lines : (q + 1) * lines, :].astype(F32) - product
        ).astype(BF16)


def invert(a_ref):
    lane = lax.broadcasted_iota(jnp.int32, (8, L), 1)
    sub = lax.broadcasted_iota(jnp.int32, (8, L), 0)
    wide_lane = lax.broadcasted_iota(jnp.int32, (L, L), 1)

    def step(k, carry):
        base = pl.multiple_of(8 * k, 8)
        panel = a_ref[pl.ds(base, 8), :]
        columns = [
            jnp.broadcast_to(
                jnp.sum(jnp.where(lane == base + j, panel, 0.0), axis=1, keepdims=True), (8, L)
            )
            for j in range(8)
        ]
        whole = a_ref[...]
        factors = [
            jnp.sum(jnp.where(wide_lane == base + j, whole, 0.0), axis=1, keepdims=True)
            for j in range(8)
        ]
        for j in range(8):
            own = columns[j]
            inverse = 1.0 / own[j : j + 1, :]
            here = sub == j
            panel = jnp.where(lane == base + j, jnp.where(here, 1.0, 0.0), panel)
            scaled = panel[j : j + 1, :] * inverse
            panel = jnp.where(here, scaled, panel - own * scaled)
            for m in range(j + 1, 8):
                scaled = columns[m][j : j + 1, :] * inverse
                columns[m] = jnp.where(here, scaled, columns[m] - own * scaled)
        inside = (wide_lane >= base) & (wide_lane < base + 8)
        rest = jnp.where(inside, 0.0, whole)
        for j in range(8):
            rest = rest - factors[j] * panel[j : j + 1, :]
        a_ref[...] = rest
        a_ref[pl.ds(base, 8), :] = panel
        return carry

    lax.fori_loop(0, L // 8, step, 0)


def fourth_kernel(
    c_ref, twice_ref, low_ref, comp_ref, a_ref, gm_ref, gc_ref, q_ref, st_ref
):
    n = c_ref.shape[0]
    tile = gc_ref.shape[0]
    thin, cut, groups, wide = B // n, L // n, tile // B, tile // L
    for p in range(n):
        a_ref[p * cut : (p + 1) * cut, :] = c_ref[p, 0:cut, :]
        at = cut
        gm_ref[p * thin : (p + 1) * thin, :] = c_ref[p, at : at + thin, :]
        at += thin
        for w in range(2):
            q_ref[p * thin : (p + 1) * thin, w * L : (w + 1) * L] = c_ref[p, at : at + thin, :]
            at += thin
        for s in range(groups):
            gc_ref[s * B + p * thin : s * B + (p + 1) * thin, :] = c_ref[p, at : at + thin, :]
            at += thin
        for w in range(wide):
            st_ref[p * thin : (p + 1) * thin, w * L : (w + 1) * L] = c_ref[p, at : at + thin, :]
            at += thin
    inner = a_ref[...]
    same = lax.broadcasted_iota(jnp.int32, (L, L), 0) == lax.broadcasted_iota(
        jnp.int32, (L, L), 1
    )
    a_ref[...] = jnp.where(same, 1.0, 0.0) + 0.5 * (inner + inner.T)
    invert(a_ref)
    x = a_ref[...]
    block_right = gm_ref[...]
    right = gc_ref[...]
    half = dot(block_right, x)
    solved = dot(right, x)
    high = solved.astype(BF16)
    twice_ref[:, 0:L] = high
    twice_ref[:, L:] = high
    low_ref[...] = (solved - high.astype(F32)).astype(BF16)
    square = q_ref[...] - dot_nt(half, block_right)
    square = 0.5 * (square + square.T)
    a_ref[...] = square[:L, :L]
    st_ref[...] = st_ref[...] - dot_nt(half, right)
    invert(a_ref)
    u = a_ref[...]
    v = dot(square[L:, :L], u)
    a_ref[...] = square[L:, L:] - dot(v, square[:L, L:])
    top = st_ref[0:L, :]
    first = dot(u, top)
    second = st_ref[L:, :] - dot(v, top)
    invert(a_ref)
    second = dot(a_ref[...], second)
    comp_ref[0:L, :] = (first - dot(v.T, second)).astype(BF16)
    comp_ref[L:, :] = second.astype(BF16)


VMEM = pl.BlockSpec(memory_space=pltpu.VMEM)
PARAMS = pltpu.CompilerParams(vmem_limit_bytes=10 * 2**20)
FIRST_PARAMS = pltpu.CompilerParams(vmem_limit_bytes=58 * 2**20)
LAST_PARAMS = pltpu.CompilerParams(vmem_limit_bytes=51 * 2**20)
SMEM = pl.BlockSpec(memory_space=pltpu.SMEM)
HBM = pl.BlockSpec(memory_space=pltpu.HBM)


def of(shape, dtype=F32):
    return jax.ShapeDtypeStruct(shape, dtype)


def all_steps(inv_hessian, weights, calib, block):
    tile = inv_hessian.shape[0]
    n = lax.axis_size(ROW)
    count = lax.axis_size("z")
    lines = weights.shape[0] // n
    thin, cut, groups, wide = B // n, L // n, tile // B, tile // L
    rows = groups * thin
    strip_rows = wide * thin
    small_rows = cut + 3 * thin
    sent, keep, give = pl.pallas_call(
        first_kernel,
        out_shape=(
            of((n, rows + cut + strip_rows, L)),
            of((count, lines, B), BF16),
            of((count, lines, B), BF16),
        ),
        in_specs=[SMEM, HBM, HBM, HBM],
        out_specs=(VMEM, VMEM, VMEM),
        scratch_shapes=[
            pltpu.VMEM((tile, tile), F32),
            pltpu.VMEM((L, tile), BF16),
            pltpu.VMEM((L, tile), BF16),
            pltpu.SemaphoreType.DMA((4 + groups,)),
        ],
        compiler_params=FIRST_PARAMS,
        name="first",
    )(block, inv_hessian, calib, weights.reshape(n, lines, tile))
    arrived = exchanged(sent, ROW)
    got = lax.ppermute(give, "core", [(0, 1), (1, 0)])
    turned = pl.pallas_call(
        partial(choose_kernel, groups=groups),
        out_shape=(of((lines, B), BF16),) * count,
        in_specs=[SMEM, VMEM, VMEM],
        out_specs=(VMEM,) * count,
        compiler_params=PARAMS,
        name="choose",
    )(block, keep, got)
    early = count // 2 + 1
    shifted = [turned[0]]
    for k in range(1, count):
        perm = [(i, (i + k) % count) for i in range(count)]
        shifted.append(lax.ppermute(turned[k], "z", perm))
    small, piece, strip, window = pl.pallas_call(
        partial(second_kernel, count=count),
        out_shape=(
            of((small_rows, L)),
            of((rows, L)),
            of((strip_rows, L)),
            of((lines, B), BF16),
        ),
        in_specs=[SMEM] + [VMEM] * (1 + early),
        out_specs=(VMEM, VMEM, VMEM, VMEM),
        compiler_params=PARAMS,
        name="second",
    )(block, arrived, *shifted[:early])
    turn = [(i * n + j, j * n + i) for i in range(n) for j in range(n)]
    turned = lax.ppermute(piece, (*ROW, *COL), turn)
    gathered = lax.all_gather(small, COL)
    sent = pl.pallas_call(
        third_kernel,
        out_shape=of((n, small_rows + rows + strip_rows, L)),
        in_specs=[SMEM, VMEM, VMEM, VMEM],
        out_specs=VMEM,
        compiler_params=PARAMS,
        name="third",
    )(block, gathered, piece, strip)
    arrived = exchanged(sent, ROW)
    packed = pl.pallas_call(
        partial(pack_kernel, groups=groups),
        out_shape=of((count, lines + rows, B), BF16),
        in_specs=[SMEM] + [VMEM] * (2 + count - early),
        out_specs=VMEM,
        scratch_shapes=[pltpu.VMEM((lines, B), BF16)],
        compiler_params=PARAMS,
        name="pack",
    )(block, window, turned, *shifted[early:])
    packed = exchanged(packed, "z")
    other = lax.ppermute(packed, "core", [(0, 1), (1, 0)])
    twice, low, comp = pl.pallas_call(
        fourth_kernel,
        out_shape=(of((tile, 2 * L), BF16), of((tile, L), BF16), of((B, tile), BF16)),
        in_specs=[VMEM],
        out_specs=(VMEM, VMEM, VMEM),
        scratch_shapes=[
            pltpu.VMEM((L, L), F32),
            pltpu.VMEM((B, L), F32),
            pltpu.VMEM((tile, L), F32),
            pltpu.VMEM((B, B), F32),
            pltpu.VMEM((B, tile), F32),
        ],
        cost_estimate=pl.CostEstimate(
            flops=20_000_000_000, bytes_accessed=4_000_000, transcendentals=0
        ),
        compiler_params=PARAMS,
        name="fourth",
    )(arrived)
    steps = 4
    return pl.pallas_call(
        last_kernel,
        grid=(steps,),
        out_shape=(of((tile, tile)), of((n * lines, tile), BF16)),
        in_specs=[
            pl.BlockSpec((tile // steps, tile), lambda i: (i, 0)),
            pl.BlockSpec((n * lines // steps, tile), lambda i: (i, 0)),
            VMEM,
            VMEM,
            VMEM,
            VMEM,
            VMEM,
        ],
        out_specs=(
            pl.BlockSpec((tile // steps, tile), lambda i: (i, 0)),
            pl.BlockSpec((n * lines // steps, tile), lambda i: (i, 0)),
        ),
        scratch_shapes=[pltpu.VMEM((tile, 2 * L), BF16), pltpu.VMEM((n, lines, B), BF16)],
        compiler_params=LAST_PARAMS,
        name="last",
    )(inv_hessian, weights, packed, other, twice, low, comp)


def solution(mesh):
    finer = Mesh(mesh.devices.reshape(4, 4, 8, 2), (*ROW, *COL))
    specs = (P(ROW, COL), P(ROW, COL), P(), P())
    return jax.shard_map(
        all_steps, mesh=finer, in_specs=specs, out_specs=specs[:2], check_vma=False
    )
```

```python
from functools import partial

import jax
import jax.numpy as jnp
from jax import lax
from jax.experimental import pallas as pl
from jax.experimental.pallas import tpu as pltpu
from jax.sharding import Mesh
from jax.sharding import PartitionSpec as P

B = 256
L = 128
ROW = ("x", "y")
COL = ("z", "core")
F32 = jnp.float32
BF16 = jnp.bfloat16
HIGHEST = lax.Precision.HIGHEST


def exchanged(parts, axis):
    return lax.all_to_all(parts, axis, split_axis=0, concat_axis=0, tiled=True)


def dot(a, b, dims=((1,), (0,))):
    return lax.dot_general(a, b, (dims, ((), ())), precision=HIGHEST, preferred_element_type=F32)


def dot_nt(a, b):
    return dot(a, b, ((1,), (1,)))


def in_three(x):
    first = x.astype(BF16)
    rest = x - first.astype(F32)
    second = rest.astype(BF16)
    third = (rest - second.astype(F32)).astype(BF16)
    return first, second, third


def place_of(block_ref, groups):
    owner = block_ref[0] // groups
    return owner, block_ref[0] - owner * groups


def first_kernel(
    block_ref, source_ref, calib_ref, w_ref, sent_ref, keep_ref, give_ref,
    h_ref, rows_ref, cols_ref, sems,
):
    n = sent_ref.shape[0]
    half = keep_ref.shape[0]
    tile = h_ref.shape[1]
    groups, wide, thin = tile // B, tile // L, B // n
    _, sub = place_of(block_ref, groups)
    row = lax.axis_index("x") * lax.axis_size("y") + lax.axis_index("y")
    core = lax.axis_index("core")
    col = lax.axis_index("z") * lax.axis_size("core") + core
    offset = pl.multiple_of(sub * B, B)

    def window_of(which):
        return w_ref.at[pl.ds(which * half, half), :, pl.ds(offset, B)]

    copies = [
        pltpu.make_async_copy(
            calib_ref.at[:, pl.ds(pl.multiple_of(row * tile, L), tile)], rows_ref, sems.at[0]
        ),
        pltpu.make_async_copy(
            calib_ref.at[:, pl.ds(pl.multiple_of(col * tile, L), tile)], cols_ref, sems.at[1]
        ),
        pltpu.make_async_copy(window_of(core), keep_ref, sems.at[2]),
        pltpu.make_async_copy(window_of(1 - core), give_ref, sems.at[3]),
    ]
    blocks = [
        pltpu.make_async_copy(
            source_ref.at[g * B : (g + 1) * B, :], h_ref.at[g * B : (g + 1) * B, :], sems.at[4 + g]
        )
        for g in range(groups)
    ]
    copies[0].start()
    blocks[0].start()
    copies[1].start()
    for copy in blocks[1:] + copies[2:]:
        copy.start()
    copies[0].wait()
    left = None
    for g in range(groups):
        blocks[g].wait()
        rows = rows_ref[:, g * B : (g + 1) * B]
        for part in in_three(h_ref[g * B : (g + 1) * B, :]):
            more = jnp.dot(rows, part, preferred_element_type=F32)
            left = more if left is None else left + more
    copies[1].wait()
    right = left.T
    cols = cols_ref[...]
    dims = (((1,), (1,)), ((), ()))
    first, second, third = in_three(left)
    inner = lax.dot_general(first, cols, dims, preferred_element_type=F32)
    inner += lax.dot_general(second, cols, dims, preferred_element_type=F32)
    inner += lax.dot_general(third, cols, dims, preferred_element_type=F32)
    cut = L // n
    for p in range(n):
        for s in range(groups):
            at = s * B + p * thin
            sent_ref[p, s * thin : (s + 1) * thin, :] = right[at : at + thin]
        at = groups * thin
        sent_ref[p, at : at + cut, :] = inner[p * cut : (p + 1) * cut]
        at += cut
        for w in range(wide):
            sent_ref[p, at + w * thin : at + (w + 1) * thin, :] = h_ref[
                pl.ds(pl.multiple_of(offset + p * thin, thin), thin), w * L : (w + 1) * L
            ]
    copies[2].wait()
    copies[3].wait()


def choose_kernel(block_ref, keep_ref, got_ref, *turned_refs, groups):
    count = len(turned_refs)
    owner, _ = place_of(block_ref, groups)
    z = lax.axis_index("z")
    own = owner % 2 == lax.axis_index("core")
    for k in range(count):
        at = (z + k) % count
        turned_refs[k][...] = jnp.where(own, keep_ref[at], got_ref[at])


def pick_shifted(block_ref, shifted, window_ref, groups, count, first=0):
    owner, _ = place_of(block_ref, groups)
    away = (lax.axis_index("z") + count - owner // 2) % count
    for k, ref in enumerate(shifted):

        @pl.when(away == first + k)
        def _(ref=ref):
            window_ref[...] = ref[...]


def second_kernel(block_ref, arrived_ref, *refs, count):
    *shifted, small_ref, piece_ref, strip_ref, window_ref = refs
    n = arrived_ref.shape[0]
    rows = piece_ref.shape[0]
    thin, cut = B // n, L // n
    owner, sub = place_of(block_ref, rows // thin)
    pick_shifted(block_ref, shifted, window_ref, rows // thin, count)
    total = arrived_ref[0, 0 : rows + cut, :]
    for p in range(1, n):
        total = total + arrived_ref[p, 0 : rows + cut, :]
    piece_ref[...] = total[:rows]
    strip_ref[...] = arrived_ref[owner, rows + cut :, :]
    small_ref[0:cut] = total[rows:]
    small_ref[cut : cut + thin] = piece_ref[pl.ds(pl.multiple_of(sub * thin, thin), thin), :]
    small_ref[cut + thin :] = strip_ref[
        pl.ds(pl.multiple_of(2 * sub * thin, 2 * thin), 2 * thin), :
    ]


def third_kernel(block_ref, gathered_ref, piece_ref, strip_ref, sent_ref):
    n, small, _ = gathered_ref.shape
    rows = piece_ref.shape[0]
    cut = L // n
    owner, _ = place_of(block_ref, rows * n // B)
    total = gathered_ref[0, 0:cut, :]
    for p in range(1, n):
        total = total + gathered_ref[p, 0:cut, :]
    chosen = gathered_ref[owner, cut:small, :]
    piece, strip = piece_ref[...], strip_ref[...]
    for p in range(n):
        sent_ref[p, 0:cut, :] = total
        sent_ref[p, cut:small, :] = chosen
        sent_ref[p, small : small + rows, :] = piece
        sent_ref[p, small + rows :, :] = strip


def pack_kernel(block_ref, window_ref, turned_ref, *refs, groups):
    *shifted, sent_ref, chosen_ref = refs
    lines = window_ref.shape[0]
    count = sent_ref.shape[0]
    chosen_ref[...] = window_ref[...]
    pick_shifted(block_ref, shifted, chosen_ref, groups, count, count - len(shifted))
    window = chosen_ref[...]
    turned = turned_ref[...]
    first = turned.astype(BF16)
    second = (turned - first.astype(F32)).astype(BF16)
    for p in range(count):
        sent_ref[p, 0:lines, :] = window
        sent_ref[p, lines:, 0:L] = first
        sent_ref[p, lines:, L:] = second


def last_kernel(core_ref, h_ref, w_ref, half_ref, high_ref, low_ref, comp_ref, *refs):
    updated_ref, pruned_ref, right_ref = refs[-3:]
    count, lines, _ = half_ref.shape
    step = pl.program_id(0)
    pairs, _, thin, tile = h_ref.shape
    groups = tile // B
    lines -= groups * thin

    @pl.when(step == 0)
    def _():
        for z in range(count):
            for s in range(groups):
                at = (s * count + z) * thin
                right_ref[at : at + thin, :] = half_ref[
                    z, lines + s * thin : lines + (s + 1) * thin, :
                ]

    part = pairs * thin
    right = right_ref[pl.ds(pl.multiple_of(step * part, 16), part), :]
    dims = (((1,), (1,)), ((), ()))
    change = lax.dot_general(right[:, L:], high_ref[...], dims, preferred_element_type=F32)
    change += lax.dot_general(right[:, :L], high_ref[...], dims, preferred_element_type=F32)
    change += lax.dot_general(right[:, :L], low_ref[...], dims, preferred_element_type=F32)
    for q in range(pairs):
        updated_ref[q, 0] = h_ref[q, 0] - change[q * thin : (q + 1) * thin]
    some = w_ref.shape[1]
    comp = comp_ref[...]
    for q in range(some):
        window = half_ref[step * some + q, 0:lines, :]
        product = jnp.dot(window, comp, preferred_element_type=F32)
        pruned_ref[0, q] = (w_ref[0, q].astype(F32) - product).astype(BF16)


def last_part(core, h, w, half, high, low, comp, done=()):
    steps = 4
    pairs, _, thin, tile = h.shape
    _, count, lines, _ = w.shape
    h_spec = pl.BlockSpec((pairs // steps, 1, thin, tile), lambda i, c: (i, c[0], 0, 0))
    w_spec = pl.BlockSpec((1, count // steps, lines, tile), lambda i, c: (c[0], i, 0, 0))
    return pl.pallas_call(
        last_kernel,
        grid_spec=pltpu.PrefetchScalarGridSpec(
            num_scalar_prefetch=1,
            grid=(steps,),
            in_specs=[h_spec, w_spec, VMEM, VMEM, VMEM, VMEM] + [HBM] * len(done),
            out_specs=(h_spec, w_spec),
            scratch_shapes=[pltpu.VMEM((pairs * thin, 2 * L), BF16)],
        ),
        out_shape=(of(h.shape), of(w.shape, BF16)),
        input_output_aliases={7 + k: k for k in range(len(done))},
        compiler_params=LAST_PARAMS,
        name="last",
    )(core, h, w, half, high, low, comp, *done)


def invert(a_ref):
    lane = lax.broadcasted_iota(jnp.int32, (8, L), 1)
    sub = lax.broadcasted_iota(jnp.int32, (8, L), 0)
    wide_lane = lax.broadcasted_iota(jnp.int32, (L, L), 1)

    def step(k, carry):
        base = pl.multiple_of(8 * k, 8)
        panel = a_ref[pl.ds(base, 8), :]
        columns = [
            jnp.broadcast_to(
                jnp.sum(jnp.where(lane == base + j, panel, 0.0), axis=1, keepdims=True), (8, L)
            )
            for j in range(8)
        ]
        whole = a_ref[...]
        factors = [
            jnp.sum(jnp.where(wide_lane == base + j, whole, 0.0), axis=1, keepdims=True)
            for j in range(8)
        ]
        for j in range(8):
            own = columns[j]
            inverse = 1.0 / own[j : j + 1, :]
            here = sub == j
            panel = jnp.where(lane == base + j, jnp.where(here, 1.0, 0.0), panel)
            scaled = panel[j : j + 1, :] * inverse
            panel = jnp.where(here, scaled, panel - own * scaled)
            for m in range(j + 1, 8):
                scaled = columns[m][j : j + 1, :] * inverse
                columns[m] = jnp.where(here, scaled, columns[m] - own * scaled)
        inside = (wide_lane >= base) & (wide_lane < base + 8)
        rest = jnp.where(inside, 0.0, whole)
        for j in range(8):
            rest = rest - factors[j] * panel[j : j + 1, :]
        a_ref[...] = rest
        a_ref[pl.ds(base, 8), :] = panel
        return carry

    lax.fori_loop(0, L // 8, step, 0)


def fourth_kernel(
    c_ref, high_ref, low_ref, comp_ref, a_ref, gm_ref, gc_ref, q_ref, st_ref
):
    n = c_ref.shape[0]
    tile = gc_ref.shape[0]
    thin, cut, groups, wide = B // n, L // n, tile // B, tile // L
    for p in range(n):
        a_ref[p * cut : (p + 1) * cut, :] = c_ref[p, 0:cut, :]
        at = cut
        gm_ref[p * thin : (p + 1) * thin, :] = c_ref[p, at : at + thin, :]
        at += thin
        for w in range(2):
            q_ref[p * thin : (p + 1) * thin, w * L : (w + 1) * L] = c_ref[p, at : at + thin, :]
            at += thin
        for s in range(groups):
            gc_ref[s * B + p * thin : s * B + (p + 1) * thin, :] = c_ref[p, at : at + thin, :]
            at += thin
        for w in range(wide):
            st_ref[p * thin : (p + 1) * thin, w * L : (w + 1) * L] = c_ref[p, at : at + thin, :]
            at += thin
    inner = a_ref[...]
    same = lax.broadcasted_iota(jnp.int32, (L, L), 0) == lax.broadcasted_iota(
        jnp.int32, (L, L), 1
    )
    a_ref[...] = jnp.where(same, 1.0, 0.0) + 0.5 * (inner + inner.T)
    invert(a_ref)
    x = a_ref[...]
    block_right = gm_ref[...]
    right = gc_ref[...]
    half = dot(block_right, x)
    solved = dot(right, x)
    high = solved.astype(BF16)
    high_ref[...] = high
    low_ref[...] = (solved - high.astype(F32)).astype(BF16)
    square = q_ref[...] - dot_nt(half, block_right)
    square = 0.5 * (square + square.T)
    a_ref[...] = square[:L, :L]
    st_ref[...] = st_ref[...] - dot_nt(half, right)
    invert(a_ref)
    u = a_ref[...]
    v = dot(square[L:, :L], u)
    a_ref[...] = square[L:, L:] - dot(v, square[:L, L:])
    top = st_ref[0:L, :]
    first = dot(u, top)
    second = st_ref[L:, :] - dot(v, top)
    invert(a_ref)
    second = dot(a_ref[...], second)
    comp_ref[0:L, :] = (first - dot(v.T, second)).astype(BF16)
    comp_ref[L:, :] = second.astype(BF16)


VMEM = pl.BlockSpec(memory_space=pltpu.VMEM)
PARAMS = pltpu.CompilerParams(vmem_limit_bytes=10 * 2**20)
FIRST_PARAMS = pltpu.CompilerParams(vmem_limit_bytes=58 * 2**20)
LAST_PARAMS = pltpu.CompilerParams(vmem_limit_bytes=51 * 2**20)
SMEM = pl.BlockSpec(memory_space=pltpu.SMEM)
HBM = pl.BlockSpec(memory_space=pltpu.HBM)


def of(shape, dtype=F32):
    return jax.ShapeDtypeStruct(shape, dtype)


def all_steps(inv_hessian, weights, calib, block):
    tile = inv_hessian.shape[0]
    n = lax.axis_size(ROW)
    count = lax.axis_size("z")
    lines = weights.shape[0] // n
    thin, cut, groups, wide = B // n, L // n, tile // B, tile // L
    rows = groups * thin
    strip_rows = wide * thin
    small_rows = cut + 3 * thin
    sent, keep, give = pl.pallas_call(
        first_kernel,
        out_shape=(
            of((n, rows + cut + strip_rows, L)),
            of((count, lines, B), BF16),
            of((count, lines, B), BF16),
        ),
        in_specs=[SMEM, HBM, HBM, HBM],
        out_specs=(VMEM, VMEM, VMEM),
        scratch_shapes=[
            pltpu.VMEM((tile, tile), F32),
            pltpu.VMEM((L, tile), BF16),
            pltpu.VMEM((L, tile), BF16),
            pltpu.SemaphoreType.DMA((4 + groups,)),
        ],
        compiler_params=FIRST_PARAMS,
        name="first",
    )(block, inv_hessian, calib, weights.reshape(n, lines, tile))
    arrived = exchanged(sent, ROW)
    got = lax.ppermute(give, "core", [(0, 1), (1, 0)])
    turned = pl.pallas_call(
        partial(choose_kernel, groups=groups),
        out_shape=(of((lines, B), BF16),) * count,
        in_specs=[SMEM, VMEM, VMEM],
        out_specs=(VMEM,) * count,
        compiler_params=PARAMS,
        name="choose",
    )(block, keep, got)
    early = count // 2
    shifted = [turned[0]]
    for k in range(1, count):
        perm = [(i, (i + k) % count) for i in range(count)]
        shifted.append(lax.ppermute(turned[k], "z", perm))
    small, piece, strip, window = pl.pallas_call(
        partial(second_kernel, count=count),
        out_shape=(
            of((small_rows, L)),
            of((rows, L)),
            of((strip_rows, L)),
            of((lines, B), BF16),
        ),
        in_specs=[SMEM] + [VMEM] * (1 + early),
        out_specs=(VMEM, VMEM, VMEM, VMEM),
        compiler_params=PARAMS,
        name="second",
    )(block, arrived, *shifted[:early])
    turn = [(i * n + j, j * n + i) for i in range(n) for j in range(n)]
    turned = lax.ppermute(piece, (*ROW, *COL), turn)
    gathered = lax.all_gather(small, COL)
    sent = pl.pallas_call(
        third_kernel,
        out_shape=of((n, small_rows + rows + strip_rows, L)),
        in_specs=[SMEM, VMEM, VMEM, VMEM],
        out_specs=VMEM,
        compiler_params=PARAMS,
        name="third",
    )(block, gathered, piece, strip)
    arrived = exchanged(sent, ROW)
    packed = pl.pallas_call(
        partial(pack_kernel, groups=groups),
        out_shape=of((count, lines + rows, B), BF16),
        in_specs=[SMEM] + [VMEM] * (2 + count - early),
        out_specs=VMEM,
        scratch_shapes=[pltpu.VMEM((lines, B), BF16)],
        compiler_params=PARAMS,
        name="pack",
    )(block, window, turned, *shifted[early:])
    packed = exchanged(packed, "z")
    other = lax.ppermute(packed, "core", [(0, 1), (1, 0)])
    high, low, comp = pl.pallas_call(
        fourth_kernel,
        out_shape=(of((tile, L), BF16), of((tile, L), BF16), of((B, tile), BF16)),
        in_specs=[VMEM],
        out_specs=(VMEM, VMEM, VMEM),
        scratch_shapes=[
            pltpu.VMEM((L, L), F32),
            pltpu.VMEM((B, L), F32),
            pltpu.VMEM((tile, L), F32),
            pltpu.VMEM((B, B), F32),
            pltpu.VMEM((B, tile), F32),
        ],
        cost_estimate=pl.CostEstimate(
            flops=20_000_000_000, bytes_accessed=4_000_000, transcendentals=0
        ),
        compiler_params=PARAMS,
        name="fourth",
    )(arrived)
    core = lax.axis_index("core").astype(jnp.int32).reshape(1)
    h = inv_hessian.reshape(groups * count, 2, thin, tile)
    w = weights.reshape(2, count, lines, tile)
    done = last_part(core, h, w, packed, high, low, comp)
    updated, pruned = last_part(1 - core, h, w, other, high, low, comp, done)
    return (updated.reshape(tile, tile), pruned.reshape(n * lines, tile))


def solution(mesh):
    finer = Mesh(mesh.devices.reshape(4, 4, 8, 2), (*ROW, *COL))
    specs = (P(ROW, COL), P(ROW, COL), P(), P())
    return jax.shard_map(
        all_steps, mesh=finer, in_specs=specs, out_specs=specs[:2], check_vma=False
    )
```

```python
from functools import partial

import jax
import jax.numpy as jnp
from jax import lax
from jax.experimental import pallas as pl
from jax.experimental.pallas import tpu as pltpu
from jax.sharding import Mesh
from jax.sharding import PartitionSpec as P

B = 256
L = 128
ROW = ("x", "y")
COL = ("z", "core")
F32 = jnp.float32
BF16 = jnp.bfloat16
HIGHEST = lax.Precision.HIGHEST


def exchanged(parts, axis):
    return lax.all_to_all(parts, axis, split_axis=0, concat_axis=0, tiled=True)


def dot(a, b, dims=((1,), (0,))):
    return lax.dot_general(a, b, (dims, ((), ())), precision=HIGHEST, preferred_element_type=F32)


def dot_nt(a, b):
    return dot(a, b, ((1,), (1,)))


def in_three(x):
    first = x.astype(BF16)
    rest = x - first.astype(F32)
    second = rest.astype(BF16)
    third = (rest - second.astype(F32)).astype(BF16)
    return first, second, third


def place_of(block_ref, groups):
    owner = block_ref[0] // groups
    return owner, block_ref[0] - owner * groups


def first_kernel(
    block_ref, source_ref, calib_ref, w_ref, sent_ref, keep_ref, give_ref,
    h_ref, rows_ref, cols_ref, sems,
):
    n = sent_ref.shape[0]
    half = keep_ref.shape[0]
    tile = h_ref.shape[1]
    groups, wide, thin = tile // B, tile // L, B // n
    _, sub = place_of(block_ref, groups)
    row = lax.axis_index("x") * lax.axis_size("y") + lax.axis_index("y")
    core = lax.axis_index("core")
    col = lax.axis_index("z") * lax.axis_size("core") + core
    offset = pl.multiple_of(sub * B, B)

    def window_of(which):
        return w_ref.at[pl.ds(which * half, half), :, pl.ds(offset, B)]

    copies = [
        pltpu.make_async_copy(
            calib_ref.at[:, pl.ds(pl.multiple_of(row * tile, L), tile)], rows_ref, sems.at[0]
        ),
        pltpu.make_async_copy(
            calib_ref.at[:, pl.ds(pl.multiple_of(col * tile, L), tile)], cols_ref, sems.at[1]
        ),
        pltpu.make_async_copy(window_of(core), keep_ref, sems.at[2]),
        pltpu.make_async_copy(window_of(1 - core), give_ref, sems.at[3]),
    ]
    blocks = [
        pltpu.make_async_copy(
            source_ref.at[g * B : (g + 1) * B, :], h_ref.at[g * B : (g + 1) * B, :], sems.at[4 + g]
        )
        for g in range(groups)
    ]
    copies[0].start()
    blocks[0].start()
    copies[1].start()
    for copy in blocks[1:] + copies[2:]:
        copy.start()
    copies[0].wait()
    left = None
    for g in range(groups):
        blocks[g].wait()
        rows = rows_ref[:, g * B : (g + 1) * B]
        for part in in_three(h_ref[g * B : (g + 1) * B, :]):
            more = jnp.dot(rows, part, preferred_element_type=F32)
            left = more if left is None else left + more
    copies[1].wait()
    right = left.T
    cols = cols_ref[...]
    dims = (((1,), (1,)), ((), ()))
    first, second, third = in_three(left)
    inner = lax.dot_general(first, cols, dims, preferred_element_type=F32)
    inner += lax.dot_general(second, cols, dims, preferred_element_type=F32)
    inner += lax.dot_general(third, cols, dims, preferred_element_type=F32)
    cut = L // n
    for p in range(n):
        for s in range(groups):
            at = s * B + p * thin
            sent_ref[p, s * thin : (s + 1) * thin, :] = right[at : at + thin]
        at = groups * thin
        sent_ref[p, at : at + cut, :] = inner[p * cut : (p + 1) * cut]
        at += cut
        for w in range(wide):
            sent_ref[p, at + w * thin : at + (w + 1) * thin, :] = h_ref[
                pl.ds(pl.multiple_of(offset + p * thin, thin), thin), w * L : (w + 1) * L
            ]
    copies[2].wait()
    copies[3].wait()


def choose_kernel(block_ref, keep_ref, got_ref, *turned_refs, groups):
    count = len(turned_refs)
    owner, _ = place_of(block_ref, groups)
    z = lax.axis_index("z")
    own = owner % 2 == lax.axis_index("core")
    for k in range(count):
        at = (z + k) % count
        turned_refs[k][...] = jnp.where(own, keep_ref[at], got_ref[at])


def pick_shifted(block_ref, shifted, window_ref, groups, count, first=0):
    owner, _ = place_of(block_ref, groups)
    away = (lax.axis_index("z") + count - owner // 2) % count
    for k, ref in enumerate(shifted):

        @pl.when(away == first + k)
        def _(ref=ref):
            window_ref[...] = ref[...]


def second_kernel(block_ref, arrived_ref, *refs, count):
    *shifted, small_ref, piece_ref, strip_ref, window_ref = refs
    n = arrived_ref.shape[0]
    rows = piece_ref.shape[0]
    thin, cut = B // n, L // n
    owner, sub = place_of(block_ref, rows // thin)
    pick_shifted(block_ref, shifted, window_ref, rows // thin, count)
    total = arrived_ref[0, 0 : rows + cut, :]
    for p in range(1, n):
        total = total + arrived_ref[p, 0 : rows + cut, :]
    piece_ref[...] = total[:rows]
    strip_ref[...] = arrived_ref[owner, rows + cut :, :]
    small_ref[0:cut] = total[rows:]
    small_ref[cut : cut + thin] = piece_ref[pl.ds(pl.multiple_of(sub * thin, thin), thin), :]
    small_ref[cut + thin :] = strip_ref[
        pl.ds(pl.multiple_of(2 * sub * thin, 2 * thin), 2 * thin), :
    ]


def third_kernel(block_ref, gathered_ref, piece_ref, strip_ref, sent_ref):
    n, small, _ = gathered_ref.shape
    rows = piece_ref.shape[0]
    cut = L // n
    owner, _ = place_of(block_ref, rows * n // B)
    total = gathered_ref[0, 0:cut, :]
    for p in range(1, n):
        total = total + gathered_ref[p, 0:cut, :]
    chosen = gathered_ref[owner, cut:small, :]
    piece, strip = piece_ref[...], strip_ref[...]
    for p in range(n):
        sent_ref[p, 0:cut, :] = total
        sent_ref[p, cut:small, :] = chosen
        sent_ref[p, small : small + rows, :] = piece
        sent_ref[p, small + rows :, :] = strip


def pack_kernel(block_ref, window_ref, turned_ref, *refs, groups):
    *shifted, sent_ref, chosen_ref = refs
    lines = window_ref.shape[0]
    count = sent_ref.shape[0]
    chosen_ref[...] = window_ref[...]
    pick_shifted(block_ref, shifted, chosen_ref, groups, count, count - len(shifted))
    window = chosen_ref[...]
    turned = turned_ref[...]
    first = turned.astype(BF16)
    second = (turned - first.astype(F32)).astype(BF16)
    for p in range(count):
        sent_ref[p, 0:lines, :] = window
        sent_ref[p, lines:, 0:L] = first
        sent_ref[p, lines:, L:] = second


def last_kernel(
    h_ref, w_ref, own_ref, other_ref, twice_ref, low_ref, comp_ref, updated_ref, pruned_ref,
    right_ref, window_ref,
):
    count, lines, _ = own_ref.shape
    step = pl.program_id(0)
    tile = right_ref.shape[0]
    thin = B // (2 * count)
    groups = tile // B
    lines -= groups * thin

    @pl.when(step == 0)
    def _():
        core = lax.axis_index("core")
        for ref, c in ((own_ref, core), (other_ref, 1 - core)):
            for z in range(count):
                window_ref[c * count + z] = ref[z, 0:lines, :]
                for s in range(groups):
                    at = s * B + (2 * z + c) * thin
                    right_ref[pl.ds(pl.multiple_of(at, thin), thin), :] = ref[
                        z, lines + s * thin : lines + (s + 1) * thin, :
                    ]

    part = h_ref.shape[0]
    right = right_ref[pl.ds(pl.multiple_of(step * part, 16), part), :]
    dims = (((1,), (1,)), ((), ()))
    change = lax.dot_general(right, twice_ref[...], dims, preferred_element_type=F32)
    change += lax.dot_general(right[:, :L], low_ref[...], dims, preferred_element_type=F32)
    updated_ref[...] = h_ref[...] - change
    some = w_ref.shape[0] // lines
    comp = comp_ref[...]
    window = window_ref[pl.ds(step * some, some)].reshape(some * lines, B)
    product = jnp.dot(window, comp, preferred_element_type=F32)
    pruned_ref[...] = (w_ref[...].astype(F32) - product).astype(BF16)


def invert(a_ref):
    lane = lax.broadcasted_iota(jnp.int32, (8, L), 1)
    sub = lax.broadcasted_iota(jnp.int32, (8, L), 0)
    wide_lane = lax.broadcasted_iota(jnp.int32, (L, L), 1)

    def step(k, carry):
        base = pl.multiple_of(8 * k, 8)
        panel = a_ref[pl.ds(base, 8), :]
        columns = [
            jnp.broadcast_to(
                jnp.sum(jnp.where(lane == base + j, panel, 0.0), axis=1, keepdims=True), (8, L)
            )
            for j in range(8)
        ]
        whole = a_ref[...]
        factors = [
            jnp.sum(jnp.where(wide_lane == base + j, whole, 0.0), axis=1, keepdims=True)
            for j in range(8)
        ]
        for j in range(8):
            own = columns[j]
            inverse = 1.0 / own[j : j + 1, :]
            here = sub == j
            panel = jnp.where(lane == base + j, jnp.where(here, 1.0, 0.0), panel)
            scaled = panel[j : j + 1, :] * inverse
            panel = jnp.where(here, scaled, panel - own * scaled)
            for m in range(j + 1, 8):
                scaled = columns[m][j : j + 1, :] * inverse
                columns[m] = jnp.where(here, scaled, columns[m] - own * scaled)
        inside = (wide_lane >= base) & (wide_lane < base + 8)
        rest = jnp.where(inside, 0.0, whole)
        for j in range(8):
            rest = rest - factors[j] * panel[j : j + 1, :]
        a_ref[...] = rest
        a_ref[pl.ds(base, 8), :] = panel
        return carry

    lax.fori_loop(0, L // 8, step, 0)


def fourth_kernel(
    c_ref, twice_ref, low_ref, comp_ref, a_ref, gm_ref, gc_ref, q_ref, st_ref
):
    n = c_ref.shape[0]
    tile = gc_ref.shape[0]
    thin, cut, groups, wide = B // n, L // n, tile // B, tile // L
    for p in range(n):
        a_ref[p * cut : (p + 1) * cut, :] = c_ref[p, 0:cut, :]
        at = cut
        gm_ref[p * thin : (p + 1) * thin, :] = c_ref[p, at : at + thin, :]
        at += thin
        for w in range(2):
            q_ref[p * thin : (p + 1) * thin, w * L : (w + 1) * L] = c_ref[p, at : at + thin, :]
            at += thin
        for s in range(groups):
            gc_ref[s * B + p * thin : s * B + (p + 1) * thin, :] = c_ref[p, at : at + thin, :]
            at += thin
        for w in range(wide):
            st_ref[p * thin : (p + 1) * thin, w * L : (w + 1) * L] = c_ref[p, at : at + thin, :]
            at += thin
    inner = a_ref[...]
    same = lax.broadcasted_iota(jnp.int32, (L, L), 0) == lax.broadcasted_iota(
        jnp.int32, (L, L), 1
    )
    a_ref[...] = jnp.where(same, 1.0, 0.0) + 0.5 * (inner + inner.T)
    invert(a_ref)
    x = a_ref[...]
    block_right = gm_ref[...]
    right = gc_ref[...]
    half = dot(block_right, x)
    solved = dot(right, x)
    high = solved.astype(BF16)
    twice_ref[:, 0:L] = high
    twice_ref[:, L:] = high
    low_ref[...] = (solved - high.astype(F32)).astype(BF16)
    square = q_ref[...] - dot_nt(half, block_right)
    square = 0.5 * (square + square.T)
    a_ref[...] = square[:L, :L]
    st_ref[...] = st_ref[...] - dot_nt(half, right)
    invert(a_ref)
    u = a_ref[...]
    v = dot(square[L:, :L], u)
    a_ref[...] = square[L:, L:] - dot(v, square[:L, L:])
    top = st_ref[0:L, :]
    first = dot(u, top)
    second = st_ref[L:, :] - dot(v, top)
    invert(a_ref)
    second = dot(a_ref[...], second)
    comp_ref[0:L, :] = (first - dot(v.T, second)).astype(BF16)
    comp_ref[L:, :] = second.astype(BF16)


VMEM = pl.BlockSpec(memory_space=pltpu.VMEM)
PARAMS = pltpu.CompilerParams(vmem_limit_bytes=10 * 2**20)
FIRST_PARAMS = pltpu.CompilerParams(vmem_limit_bytes=58 * 2**20)
LAST_PARAMS = pltpu.CompilerParams(vmem_limit_bytes=51 * 2**20)
SMEM = pl.BlockSpec(memory_space=pltpu.SMEM)
HBM = pl.BlockSpec(memory_space=pltpu.HBM)


def of(shape, dtype=F32):
    return jax.ShapeDtypeStruct(shape, dtype)


def all_steps(inv_hessian, weights, calib, block):
    tile = inv_hessian.shape[0]
    n = lax.axis_size(ROW)
    count = lax.axis_size("z")
    lines = weights.shape[0] // n
    thin, cut, groups, wide = B // n, L // n, tile // B, tile // L
    rows = groups * thin
    strip_rows = wide * thin
    small_rows = cut + 3 * thin
    sent, keep, give = pl.pallas_call(
        first_kernel,
        out_shape=(
            of((n, rows + cut + strip_rows, L)),
            of((count, lines, B), BF16),
            of((count, lines, B), BF16),
        ),
        in_specs=[SMEM, HBM, HBM, HBM],
        out_specs=(VMEM, VMEM, VMEM),
        scratch_shapes=[
            pltpu.VMEM((tile, tile), F32),
            pltpu.VMEM((L, tile), BF16),
            pltpu.VMEM((L, tile), BF16),
            pltpu.SemaphoreType.DMA((4 + groups,)),
        ],
        compiler_params=FIRST_PARAMS,
        name="first",
    )(block, inv_hessian, calib, weights.reshape(n, lines, tile))
    arrived = exchanged(sent, ROW)
    got = lax.ppermute(give, "core", [(0, 1), (1, 0)])
    turned = pl.pallas_call(
        partial(choose_kernel, groups=groups),
        out_shape=(of((lines, B), BF16),) * count,
        in_specs=[SMEM, VMEM, VMEM],
        out_specs=(VMEM,) * count,
        compiler_params=PARAMS,
        name="choose",
    )(block, keep, got)
    early = count // 2
    shifted = [turned[0]]
    for k in range(1, count):
        perm = [(i, (i + k) % count) for i in range(count)]
        shifted.append(lax.ppermute(turned[k], "z", perm))
    small, piece, strip, window = pl.pallas_call(
        partial(second_kernel, count=count),
        out_shape=(
            of((small_rows, L)),
            of((rows, L)),
            of((strip_rows, L)),
            of((lines, B), BF16),
        ),
        in_specs=[SMEM] + [VMEM] * (1 + early),
        out_specs=(VMEM, VMEM, VMEM, VMEM),
        compiler_params=PARAMS,
        name="second",
    )(block, arrived, *shifted[:early])
    turn = [(i * n + j, j * n + i) for i in range(n) for j in range(n)]
    turned = lax.ppermute(piece, (*ROW, *COL), turn)
    gathered = lax.all_gather(small, COL)
    sent = pl.pallas_call(
        third_kernel,
        out_shape=of((n, small_rows + rows + strip_rows, L)),
        in_specs=[SMEM, VMEM, VMEM, VMEM],
        out_specs=VMEM,
        compiler_params=PARAMS,
        name="third",
    )(block, gathered, piece, strip)
    arrived = exchanged(sent, ROW)
    packed = pl.pallas_call(
        partial(pack_kernel, groups=groups),
        out_shape=of((count, lines + rows, B), BF16),
        in_specs=[SMEM] + [VMEM] * (2 + count - early),
        out_specs=VMEM,
        scratch_shapes=[pltpu.VMEM((lines, B), BF16)],
        compiler_params=PARAMS,
        name="pack",
    )(block, window, turned, *shifted[early:])
    packed = exchanged(packed, "z")
    other = lax.ppermute(packed, "core", [(0, 1), (1, 0)])
    twice, low, comp = pl.pallas_call(
        fourth_kernel,
        out_shape=(of((tile, 2 * L), BF16), of((tile, L), BF16), of((B, tile), BF16)),
        in_specs=[VMEM],
        out_specs=(VMEM, VMEM, VMEM),
        scratch_shapes=[
            pltpu.VMEM((L, L), F32),
            pltpu.VMEM((B, L), F32),
            pltpu.VMEM((tile, L), F32),
            pltpu.VMEM((B, B), F32),
            pltpu.VMEM((B, tile), F32),
        ],
        cost_estimate=pl.CostEstimate(
            flops=20_000_000_000, bytes_accessed=4_000_000, transcendentals=0
        ),
        compiler_params=PARAMS,
        name="fourth",
    )(arrived)
    steps = 4
    return pl.pallas_call(
        last_kernel,
        grid=(steps,),
        out_shape=(of((tile, tile)), of((n * lines, tile), BF16)),
        in_specs=[
            pl.BlockSpec((tile // steps, tile), lambda i: (i, 0)),
            pl.BlockSpec((n * lines // steps, tile), lambda i: (i, 0)),
            VMEM,
            VMEM,
            VMEM,
            VMEM,
            VMEM,
        ],
        out_specs=(
            pl.BlockSpec((tile // steps, tile), lambda i: (i, 0)),
            pl.BlockSpec((n * lines // steps, tile), lambda i: (i, 0)),
        ),
        scratch_shapes=[pltpu.VMEM((tile, 2 * L), BF16), pltpu.VMEM((n, lines, B), BF16)],
        compiler_params=LAST_PARAMS,
        name="last",
    )(inv_hessian, weights, packed, other, twice, low, comp)


def solution(mesh):
    finer = Mesh(mesh.devices.reshape(4, 4, 8, 2), (*ROW, *COL))
    specs = (P(ROW, COL), P(ROW, COL), P(), P())
    return jax.shard_map(
        all_steps, mesh=finer, in_specs=specs, out_specs=specs[:2], check_vma=False
    )
```
